128 devices in a mesh: grp: 8 (over z, y_lo), slab: 16 (over y_hi, x, core).
Axes of the slice: x: 4, y: 4 (y_hi: 2, y_lo: 2; y = y_hi * 2 + y_lo), z: 4, core: 2. Of those that a mesh axis runs over, the one named last changes fastest.
Arguments:
- orbitals: float32 [16, 96, 9216], P('grp', 'slab'), may hold values from -6 to 6
- occupation: int32 [16], P('grp'), may hold values from 1 to 4
- kernel_hat: float32 [192, 36864], P('slab'), may hold values from 0.02 to 1200, as said below
- pair_mask: int32 [1], replicated, may hold values from 1 to 7
Outputs:
- exchange_terms: float32 [16, 96, 9216], P('grp', 'slab')
The draws below stay inside these ranges and needn't reach their ends.
Inputs may be any that keep to these rules, and one draw needn't show every extreme that they name: In this round group g is paired with group g XOR pair_mask. kernel_hat is positive, and unchanged when each frequency index k is replaced by (192 - k) mod 192 in all three dimensions at once.
All inputs are finite; a program needn't handle non-finite values.
Results may differ from the reference program's by a relative error of at most 0.0001.
Values sent between devices are 32-bit elements; how exact they have to be, the bound alone decides.
A program may use at most 64 MiB of HBM per device.

```python
import math
import jax
import jax.numpy as jnp
from jax import lax

G = 96
P_SIZE = 192
ORBS = 2
ORBITALS = 16
N_GRP = 8


screening = 0.0025


def draw_kernel_hat(key, part):
    factors = jax.random.uniform(key, (P_SIZE, P_SIZE, P_SIZE), jnp.float32, 0.5, 1.5)
    mirrored = jnp.roll(jnp.flip(factors, (0, 1, 2)), 1, (0, 1, 2))
    even_factors = 0.5 * (factors + mirrored)
    wave_index = jnp.arange(P_SIZE, dtype=jnp.int32)
    folded = jnp.minimum(wave_index, P_SIZE - wave_index).astype(jnp.float32)
    eigen_line = 4.0 * jnp.sin(math.pi * folded / P_SIZE) ** 2
    eigen_sum = eigen_line[:, None, None] + eigen_line[None, :, None] + eigen_line[None, None, :]
    return (even_factors / (eigen_sum + screening)).reshape(P_SIZE, P_SIZE * P_SIZE)


def plant(entries, own_key, smallest, largest):
    spot = [jax.random.randint(jax.random.fold_in(own_key, axis), (), 0, length) for axis, length in enumerate(entries.shape)]
    main_axis = entries.shape.index(max(entries.shape))
    neighbour = spot[:main_axis] + [(spot[main_axis] + 1) % entries.shape[main_axis]] + spot[main_axis + 1:]
    return entries.at[tuple(spot)].set(smallest).at[tuple(neighbour)].set(largest)


def shard_levels(rng, dims, split, least, top_value):
    def one(position, blocks):
        steps = jax.random.uniform(jax.random.fold_in(jax.random.fold_in(rng, 6), position), (blocks,), jnp.float32, least / len(split), top_value / len(split))
        return jnp.repeat(jnp.exp(steps), dims[position] // blocks).reshape((-1,) + (1,) * (len(dims) - position - 1))

    loudness = one(*split[0])
    for cut in split[1:]:
        loudness = loudness * one(*cut)
    return loudness


def scatter_about(rng, dims, scale, reach, cuts=(), kind=jnp.bfloat16):
    level = shard_levels(rng, dims, cuts, -0.22, 0.18) if cuts else 1.0
    array = jax.random.normal(rng, dims, jnp.float32) * scale * level
    return jnp.minimum(jnp.maximum(array, -reach), reach).astype(kind)


def setup_inputs(seed: int = 0) -> dict:
    key_of = jax.random.split(jax.random.key(seed), 5)
    return {
        "orbitals": scatter_about(key_of[0], (ORBITALS, G, G * G), 1.0, 6.0, ((0, 8), (1, 16)), jnp.float32),
        "occupation": plant(jax.random.randint(key_of[1], (ORBITALS,), 1, 5), jax.random.fold_in(key_of[1], 1), 1, 4).astype(jnp.int32),
        "kernel_hat": draw_kernel_hat(jax.random.fold_in(key_of[4], 71), 0),
        "pair_mask": jax.random.randint(key_of[3], (1,), 1, N_GRP).astype(jnp.int32),
    }


def pair_potential(density, kernel_half):
    padded = jnp.pad(density, ((0, G), (0, G), (0, G)))
    spectrum = jnp.fft.rfftn(padded)
    field = jnp.fft.irfftn(spectrum * kernel_half, s=(P_SIZE, P_SIZE, P_SIZE))
    return field[:G, :G, :G]


def reference(orbitals, occupation, kernel_hat, pair_mask):
    fields = orbitals.reshape(N_GRP, ORBS, G, G, G)
    weights = (0.25 * occupation.astype(jnp.float32)).reshape(N_GRP, ORBS)
    kernel_cube = kernel_hat.reshape(P_SIZE, P_SIZE, P_SIZE)
    kernel_half = jnp.transpose(kernel_cube, (2, 1, 0))[:, :, : P_SIZE // 2 + 1]
    pair_bits = pair_mask[0].astype(jnp.int32)
    high_bit = jnp.zeros((), jnp.int32)
    for shift_level in range(1, 31):
        high_bit = high_bit + (jnp.right_shift(pair_bits, shift_level) > 0).astype(jnp.int32)
    low_bits = jnp.left_shift(jnp.ones((), jnp.int32), high_bit) - 1

    def pair_step(flat_index, sums):
        flat_index = flat_index.astype(jnp.int32)
        pair_index = flat_index // (ORBS * ORBS)
        first = (flat_index // ORBS) % ORBS
        second = flat_index % ORBS
        lower_group = jnp.bitwise_or(
            jnp.left_shift(jnp.right_shift(pair_index, high_bit), high_bit + 1),
            jnp.bitwise_and(pair_index, low_bits))
        upper_group = jnp.bitwise_xor(lower_group, pair_bits)
        left_field = fields[lower_group, first]
        right_field = fields[upper_group, second]
        potential = pair_potential(left_field * right_field, kernel_half)
        sums = sums.at[lower_group, first].add(-weights[upper_group, second] * potential * right_field)
        sums = sums.at[upper_group, second].add(-weights[lower_group, first] * potential * left_field)
        return sums

    total_pairs = (N_GRP // 2) * ORBS * ORBS
    sums = lax.fori_loop(0, total_pairs, pair_step, jnp.zeros((N_GRP, ORBS, G, G, G), jnp.float32))
    return sums.reshape(N_GRP * ORBS, G, G * G)
```

```python
import math

import jax
import jax.numpy as jnp
from jax import lax
from jax.sharding import PartitionSpec as P

G = 96


def partner_swap(value, pair_bits):
    count = lax.axis_size("grp")

    def direct(mask):
        pairs = [(source, source ^ mask) for source in range(count)]
        return lambda v: lax.ppermute(v, "grp", pairs)

    return lax.switch(pair_bits - 1, [direct(mask) for mask in range(1, count)], value)


def dft_tables(size_in, size_out, period):
    row_index = lax.broadcasted_iota(jnp.int32, (size_in, size_out), 0)
    col_index = lax.broadcasted_iota(jnp.int32, (size_in, size_out), 1)
    phase_angle = (row_index * col_index % period).astype(jnp.float32) * (2.0 * math.pi / period)
    return (jnp.cos(phase_angle), jnp.sin(phase_angle))


def contract(form, left, right):
    return jnp.einsum(
        form, left, right, precision=lax.Precision.HIGH, preferred_element_type=jnp.float32
    )


def local(orbitals, occupation, kernel_hat, pair_mask):
    orbit_count = orbitals.shape[0]
    half_count = orbit_count // 2
    plane_count = orbitals.shape[1]
    grid_len = G
    padded_len = 2 * G
    kernel_cube = kernel_hat.reshape(kernel_hat.shape[0], padded_len, padded_len)
    cos_fwd, sin_fwd = dft_tables(grid_len, padded_len, padded_len)
    cos_inv, sin_inv = dft_tables(padded_len, grid_len, padded_len)
    cos_inv = cos_inv / padded_len
    sin_inv = sin_inv / padded_len
    forward_pair = jnp.stack([jnp.stack([cos_fwd, -sin_fwd]), jnp.stack([sin_fwd, cos_fwd])])
    inverse_pair = jnp.stack([jnp.stack([cos_inv, sin_inv]), jnp.stack([-sin_inv, cos_inv])])

    def line_work(pencils):
        y_spectra = contract("nckxy,cdyl->ndkxl", pencils, forward_pair)
        spectra = contract("nckxl,cdxm->ndklm", y_spectra, forward_pair)
        spectra = spectra * kernel_cube[None, None]
        x_back = contract("ncklm,cdmx->ndklx", spectra, inverse_pair)
        return contract("ncklx,cdly->ndkxy", x_back, inverse_pair)

    def packed_potential(density_pair):
        spread = contract("ncxyz,cdzk->ndkxy", density_pair, forward_pair)
        planes = lax.all_to_all(
            line_work(lax.all_to_all(spread, "slab", split_axis=2, concat_axis=3, tiled=True)),
            "slab",
            split_axis=3,
            concat_axis=2,
            tiled=True,
        )
        return contract("nckxy,cdkz->ndxyz", planes, inverse_pair)

    pair_bits = pair_mask[0]
    own_group = lax.axis_index("grp")
    partner_group = jnp.bitwise_xor(own_group, pair_bits)
    upper_side = (own_group > partner_group).astype(jnp.int32)
    weights = 0.25 * occupation.astype(jnp.float32)
    theirs, their_weights = partner_swap((orbitals, weights), pair_bits)
    paired = theirs.reshape(half_count, 2, plane_count, grid_len * grid_len)
    paired_weights = their_weights.reshape(half_count, 2)

    def add_returned(returned, parity, term):
        current = lax.dynamic_slice_in_dim(returned, parity, 1, 1)
        return lax.dynamic_update_slice_in_dim(returned, current + term[:, None], parity, 1)

    def twin_step(pair_number, loop_state):
        kept_rows, returned = loop_state
        first_row = 2 * pair_number
        second_row = first_row + 1
        own_first = lax.dynamic_index_in_dim(orbitals, first_row, 0, keepdims=False)
        own_second = lax.dynamic_index_in_dim(orbitals, second_row, 0, keepdims=False)
        weight_first = lax.dynamic_index_in_dim(weights, first_row, 0, keepdims=False)
        weight_second = lax.dynamic_index_in_dim(weights, second_row, 0, keepdims=False)
        parity_first = upper_side % 2
        parity_second = 1 - parity_first
        chosen_first = lax.dynamic_index_in_dim(paired, parity_first, 1, keepdims=False)
        chosen_second = lax.dynamic_index_in_dim(paired, parity_second, 1, keepdims=False)
        cweight_first = lax.dynamic_index_in_dim(paired_weights, parity_first, 1, keepdims=False)
        cweight_second = lax.dynamic_index_in_dim(paired_weights, parity_second, 1, keepdims=False)
        density_pair = jnp.stack(
            [own_first[None] * chosen_first, own_second[None] * chosen_second], axis=1
        )
        density_pair = density_pair.reshape(half_count, 2, plane_count, grid_len, grid_len)
        fields = packed_potential(density_pair).reshape(
            half_count, 2, plane_count, grid_len * grid_len
        )
        field_first = fields[:, 0]
        field_second = fields[:, 1]
        kept_first = -jnp.sum(cweight_first[:, None, None] * field_first * chosen_first, axis=0)
        kept_second = -jnp.sum(cweight_second[:, None, None] * field_second * chosen_second, axis=0)
        kept_rows = lax.dynamic_update_index_in_dim(kept_rows, kept_first, first_row, 0)
        kept_rows = lax.dynamic_update_index_in_dim(kept_rows, kept_second, second_row, 0)
        returned = add_returned(
            returned, parity_first, -weight_first * field_first * own_first[None]
        )
        returned = add_returned(
            returned, parity_second, -weight_second * field_second * own_second[None]
        )
        return (kept_rows, returned)

    kept_start = jnp.zeros(orbitals.shape, jnp.float32)
    returned_start = jnp.zeros((half_count, 2, plane_count, grid_len * grid_len), jnp.float32)
    kept_rows, returned = lax.fori_loop(0, half_count, twin_step, (kept_start, returned_start))
    outgoing = returned.reshape(orbit_count, plane_count, grid_len * grid_len)
    incoming = partner_swap(outgoing, pair_bits)
    return kept_rows + incoming


def solution(mesh):
    return jax.shard_map(
        local,
        mesh=mesh,
        in_specs=(P("grp", "slab", None), P("grp"), P("slab", None), P()),
        out_specs=P("grp", "slab", None),
        check_vma=False,
    )
```

```python
import functools
import math

import jax
import jax.numpy as jnp
import ml_dtypes
import numpy as np
from jax import lax
from jax.experimental import pallas as pl
from jax.experimental.pallas import tpu as pltpu
from jax.sharding import PartitionSpec as P

MESH = pl.DeviceIdType.MESH
G = 96
N = 192
PLANES = 6
CHUNKS = 3
SLABS = 16
KZ = 12
F32 = jnp.float32
BF16 = jnp.bfloat16


def halves(table):
    table = np.asarray(table, np.float64)
    high = table.astype(np.float32).astype(ml_dtypes.bfloat16)
    low = (table - high.astype(np.float64)).astype(np.float32).astype(ml_dtypes.bfloat16)
    return np.stack([high, low])


def rotation(freq, place):
    angle = 2.0 * math.pi * ((np.outer(freq, place)) % N) / N
    return np.cos(angle), np.sin(angle)


def tables():
    every = np.arange(N)
    z = np.arange(G)
    y = np.array([4 * q + r for r in range(4) for q in range(24)])
    x = np.array([PLANES * s + k for k in range(PLANES) for s in range(SLABS)])
    cos_z, sin_z = rotation(every, z)
    z_fwd = np.zeros((N, 256))
    z_fwd[:, :G], z_fwd[:, 128 : 128 + G] = cos_z, sin_z
    z_inv = np.zeros((256, 256))
    z_inv[:N, :G], z_inv[:N, 128 : 128 + G] = cos_z / N, sin_z / N
    y_fwd = np.zeros((320, 2, 2, 128))
    y_inv = np.zeros((2, 2, 128, 256))
    for parity in range(2):
        cos_y, sin_y = rotation(2 * np.arange(G) + parity, y)
        y_fwd[64:160, 0, parity, :G] = cos_y.T
        y_fwd[160:256, 0, parity, :G] = sin_y.T
        y_fwd[64:160, 1, parity, :G] = -sin_y.T
        y_fwd[160:256, 1, parity, :G] = cos_y.T
        y_inv[0, parity, :G, :G] = cos_y / N
        y_inv[1, parity, :G, :G] = -sin_y / N
        y_inv[0, parity, :G, G : 2 * G] = sin_y / N
        y_inv[1, parity, :G, G : 2 * G] = cos_y / N
    cos_x, sin_x = rotation(every, x)
    x_fwd = np.block([[cos_x, sin_x], [-sin_x, cos_x]])
    return [
        halves(value)
        for value in (z_fwd, y_fwd.reshape(320, 512), x_fwd, x_fwd.T / N, y_inv.reshape(512, 256), z_inv)
    ]


def split(value):
    high = value.astype(BF16)
    return high, (value - high.astype(F32)).astype(BF16)


def dot(left, right, contract=((1,), (0,))):
    return lax.dot_general(left, right, (contract, ((), ())), preferred_element_type=F32)


def triple(left, right, contract=((1,), (0,))):
    return (
        dot(left[0], right[0], contract)
        + dot(left[0], right[1], contract)
        + dot(left[1], right[0], contract)
    )


def kernel(
    mask,
    occ_ref, orb, kern, z_fwd, y_fwd, x_fwd, x_inv, y_inv, z_inv,
    out,
    theirs, weights, their_weights, pencils, send_a, recv_a, send_b, recv_b, spec, flat, kmat, back, landed,
    exch_s, exch_r, w_s, w_r, a_s, a_r, b_s, b_r, ret_s, ret_r, own_a, own_b,
):
    grp = lax.axis_index("grp")
    me = lax.axis_index("slab")
    partner = grp
    for bit in range(3):
        if mask >> bit & 1:
            partner = partner + (1 - 2 * (grp // 2**bit % 2)) * 2**bit
    upper = grp // 2 ** (mask.bit_length() - 1) % 2
    mine_y, mine_x, mine_c = me // 8, me // 2 % 4, me % 2

    def peer(step):
        far = 15 - step
        y, x, c = far // 8, far // 2 % 4, far % 2
        return ((mine_y + y) % 2 * 4 + (mine_x + x) % 4) * 2 + (mine_c + c) % 2

    barrier = pltpu.get_barrier_semaphore()

    def greet(step, carry):
        pl.semaphore_signal(barrier, inc=1, device_id=(grp, peer(step)), device_id_type=MESH)
        return carry

    pl.semaphore_signal(barrier, inc=1, device_id=(partner, me), device_id_type=MESH)
    lax.fori_loop(0, SLABS - 1, greet, 0)
    own_w0 = occ_ref[0].astype(F32) * 0.25
    own_w1 = occ_ref[1].astype(F32) * 0.25
    weights[0:1, :] = jnp.full((1, 128), own_w0, F32)
    weights[1:2, :] = jnp.full((1, 128), own_w1, F32)
    pl.semaphore_wait(barrier, SLABS)

    def exch_copy(c):
        rows = pl.ds(c * 288, 288)
        return pltpu.make_async_remote_copy(
            orb.at[rows], theirs.at[rows], exch_s.at[c], exch_r.at[c], device_id=(partner, me), device_id_type=MESH
        )

    for c in range(CHUNKS):
        exch_copy(c).start()
    weight_copy = pltpu.make_async_remote_copy(
        weights, their_weights, w_s, w_r, device_id=(partner, me), device_id_type=MESH
    )
    weight_copy.start()

    def flatten(step, carry):
        for sub in range(8):
            m = step * 8 + sub
            flat[pl.ds(m, KZ, stride=288), :] = kern[:, pl.ds(pl.multiple_of(m * 128, 128), 128)]
        return carry

    lax.fori_loop(0, 36, flatten, 0)

    def turn(j, carry):
        pad = jnp.zeros((32, 128), F32)
        t0, t1, t2 = [
            jnp.concatenate([flat[pl.ds(j * 288 + l, G, stride=3), :], pad], axis=0).T for l in range(3)
        ]
        base = pl.multiple_of(j * N, N)
        kmat[pl.ds(base, 128), 0:128] = t0
        kmat[pl.ds(base + 128, 64), 0:128] = t1[:64]
        kmat[pl.ds(base, 64), 128:256] = t1[64:]
        kmat[pl.ds(base + 64, 128), 128:256] = t2
        return carry

    lax.fori_loop(0, KZ, turn, 0)
    pencils[...] = jnp.zeros(pencils.shape, F32)

    def orbital(ref, c, which):
        return [ref[pl.ds(c * 288 + 2 * l + which, 48, stride=6), :] for l in range(3)]

    def block_copy(sent, landing, s_sem, r_sem, c, to):
        return pltpu.make_async_remote_copy(
            sent.at[pl.ds(c * 576 + to * 36, 36)],
            landing.at[pl.ds(c * 576 + me * 36, 36)],
            s_sem.at[c, to],
            r_sem.at[c, me],
            device_id=(grp, to),
            device_id_type=MESH,
        )

    def own_copy(sent, landing, sem, c):
        rows = pl.ds(c * 576 + me * 36, 36)
        return pltpu.make_async_copy(sent.at[rows], landing.at[rows], sem.at[c])

    def send_all(sent, landing, s_sem, r_sem, own_sem, c):
        def go(step, carry):
            block_copy(sent, landing, s_sem, r_sem, c, peer(step)).start()
            return carry

        lax.fori_loop(0, SLABS - 1, go, 0)
        own_copy(sent, landing, own_sem, c).start()

    def wait_all(sent, landing, s_sem, r_sem, own_sem, c):
        def go(step, carry):
            source = peer(step)
            pltpu.make_async_remote_copy(
                sent.at[pl.ds(c * 576 + source * 36, 36)],
                landing.at[pl.ds(c * 576 + source * 36, 36)],
                s_sem.at[c, source],
                r_sem.at[c, source],
                device_id=(grp, source),
                device_id_type=MESH,
            ).wait_recv()
            return carry

        lax.fori_loop(0, SLABS - 1, go, 0)
        own_copy(sent, landing, own_sem, c).wait()

    def forward_z(c, carry):
        exch_copy(c).wait_recv()
        first = jnp.concatenate(
            [a * b for a, b in zip(orbital(orb, c, 0), orbital(theirs, c, upper))], axis=1
        )
        second = jnp.concatenate(
            [a * b for a, b in zip(orbital(orb, c, 1), orbital(theirs, c, 1 - upper))], axis=1
        )
        for r in range(4):
            for k in range(2):
                one = first[24 * k : 24 * k + 24, G * r : G * r + G]
                two = second[24 * k : 24 * k + 24, G * r : G * r + G]
                at = k * N + r * 24
                pencils[at : at + 24, 0:G] = one
                pencils[at : at + 24, 128 : 128 + G] = two
                pencils[at + G : at + G + 24, 0:G] = two
                pencils[at + G : at + G + 24, 128 : 128 + G] = -one
        spread = triple((z_fwd[0], z_fwd[1]), split(pencils[...]), ((1,), (1,)))
        for l in range(3):
            send_a[pl.ds(c * 576 + l, N, stride=3), :] = spread[:, 128 * l : 128 * l + 128]
        send_all(send_a, recv_a, a_s, a_r, own_a, c)
        return carry

    lax.fori_loop(0, CHUNKS, forward_z, 0)

    def forward_y(c, carry):
        wait_all(send_a, recv_a, a_s, a_r, own_a, c)
        wire = jnp.concatenate([recv_a[pl.ds(c * 576 + l, N, stride=3), :] for l in range(3)], axis=1)
        high, low = split(wire)
        for k in range(2):
            lanes = slice(128 * k, 128 * k + 256)
            rows = slice(64, 320) if k == 0 else slice(0, 256)
            result = triple((high[:, lanes], low[:, lanes]), (y_fwd[0, rows], y_fwd[1, rows]))
            for l in range(4):
                spec[pl.ds(l * 1152 + (2 * c + k) * N, N), :] = result[:, 128 * l : 128 * l + 128]
        return carry

    lax.fori_loop(0, CHUNKS, forward_y, 0)

    def middle(j, carry):
        def place(d, parity, k):
            return pl.ds((2 * d + parity) * 1152 + k * N + j, SLABS, stride=KZ)

        field = jnp.concatenate(
            [
                jnp.concatenate(
                    [spec[place(d, parity, k), :] for d in range(2) for k in range(PLANES)], axis=0
                )
                for parity in range(2)
            ],
            axis=1,
        )
        spectrum = triple((x_fwd[0], x_fwd[1]), split(field))
        weight = kmat[pl.ds(pl.multiple_of(j * N, N), N), :]
        spectrum = jnp.concatenate([spectrum[:N] * weight, spectrum[N:] * weight], axis=0)
        field = triple((x_inv[0], x_inv[1]), split(spectrum))
        for parity in range(2):
            for d in range(2):
                for k in range(PLANES):
                    row = (d * PLANES + k) * SLABS
                    spec[place(d, parity, k), :] = field[row : row + SLABS, 128 * parity : 128 * parity + 128]
        return carry

    lax.fori_loop(0, KZ, middle, 0)

    def inverse_y(c, carry):
        parts = []
        for k in range(2):
            wide = jnp.concatenate(
                [spec[pl.ds(l * 1152 + (2 * c + k) * N, N), :] for l in range(4)], axis=1
            )
            parts.append(triple(split(wide), (y_inv[0], y_inv[1])))
        late = pltpu.roll(parts[1], 64, 1)
        tiles = [parts[0][:, :128], parts[0][:, 128:] + late[:, :128], late[:, 128:]]
        for l in range(3):
            send_b[pl.ds(c * 576 + l, N, stride=3), :] = tiles[l]
        send_all(send_b, recv_b, b_s, b_r, own_b, c)
        return carry

    lax.fori_loop(0, CHUNKS, inverse_y, 0)
    weight_copy.wait_recv()

    def ret_copy(c):
        rows = pl.ds(c * 288, 288)
        return pltpu.make_async_remote_copy(
            back.at[rows], landed.at[rows], ret_s.at[c], ret_r.at[c], device_id=(partner, me), device_id_type=MESH
        )

    def inverse_z(c, carry):
        wait_all(send_b, recv_b, b_s, b_r, own_b, c)
        pad = jnp.zeros((64, 128), F32)
        turned = jnp.concatenate(
            [
                jnp.concatenate([recv_b[pl.ds(c * 576 + l, N, stride=3), :], pad], axis=0).T
                for l in range(3)
            ],
            axis=0,
        )
        both = triple(split(turned), (z_inv[0], z_inv[1]))
        first, second = [], []
        for r in range(4):
            ones, twos = [], []
            for k in range(2):
                at = k * N + r * 24
                re = both[at : at + 24]
                im = both[at + G : at + G + 24]
                ones.append(re[:, :G] - im[:, 128 : 128 + G])
                twos.append(re[:, 128 : 128 + G] + im[:, :G])
            first.append(jnp.concatenate(ones, axis=0))
            second.append(jnp.concatenate(twos, axis=0))
        first = jnp.concatenate(first, axis=1)
        second = jnp.concatenate(second, axis=1)
        w_first = their_weights[pl.ds(upper, 1), :]
        w_second = their_weights[pl.ds(1 - upper, 1), :]
        for field, which, other, near, far in (
            (first, 0, upper, own_w0, w_first),
            (second, 1, 1 - upper, own_w1, w_second),
        ):
            mine, partners = orbital(orb, c, which), orbital(theirs, c, other)
            for l in range(3):
                tile = field[:, 128 * l : 128 * l + 128]
                out[pl.ds(c * 288 + 2 * l + which, 48, stride=6), :] = -(far * tile * partners[l])
                back[pl.ds(c * 288 + 2 * l + other, 48, stride=6), :] = -(near * tile * mine[l])
        ret_copy(c).start()
        return carry

    lax.fori_loop(0, CHUNKS, inverse_z, 0)

    def finish(c, carry):
        ret_copy(c).wait_recv()
        rows = pl.ds(pl.multiple_of(c * 288, 288), 288)
        out[rows, :] = out[rows, :] + landed[rows, :]
        return carry

    lax.fori_loop(0, CHUNKS, finish, 0)

    weight_copy.wait_send()
    for c in range(CHUNKS):
        exch_copy(c).wait_send()
        ret_copy(c).wait_send()

        def drain(step, carry):
            block_copy(send_a, recv_a, a_s, a_r, c, peer(step)).wait_send()
            block_copy(send_b, recv_b, b_s, b_r, c, peer(step)).wait_send()
            return carry

        lax.fori_loop(0, SLABS - 1, drain, 0)


def local(orbitals, occupation, kernel_hat, pair_mask):
    rows = orbitals.reshape(2, PLANES, 72, 128).transpose(1, 2, 0, 3).reshape(864, 128)
    consts = [jnp.asarray(value) for value in tables()]
    vmem = pl.BlockSpec(memory_space=pltpu.VMEM)
    dma = pltpu.SemaphoreType.DMA

    def branch(mask):
        def run(rows, occupation, kernel_hat, *consts):
            return pl.pallas_call(
                functools.partial(kernel, mask),
                out_shape=jax.ShapeDtypeStruct((864, 128), F32),
                in_specs=[pl.BlockSpec(memory_space=pltpu.SMEM)] + [vmem] * 8,
                out_specs=vmem,
                scratch_shapes=[
                    pltpu.VMEM((864, 128), F32),
                    pltpu.VMEM((8, 128), F32),
                    pltpu.VMEM((8, 128), F32),
                    pltpu.VMEM((384, 256), F32),
                    pltpu.VMEM((1728, 128), F32),
                    pltpu.VMEM((1728, 128), F32),
                    pltpu.VMEM((1728, 128), F32),
                    pltpu.VMEM((1728, 128), F32),
                    pltpu.VMEM((4608, 128), F32),
                    pltpu.VMEM((KZ * 288, 128), F32),
                    pltpu.VMEM((KZ * N, 256), F32),
                    pltpu.VMEM((864, 128), F32),
                    pltpu.VMEM((864, 128), F32),
                    dma((CHUNKS,)), dma((CHUNKS,)), dma, dma,
                    dma((CHUNKS, SLABS)), dma((CHUNKS, SLABS)), dma((CHUNKS, SLABS)), dma((CHUNKS, SLABS)),
                    dma((CHUNKS,)), dma((CHUNKS,)), dma((CHUNKS,)), dma((CHUNKS,)),
                ],
                compiler_params=pltpu.CompilerParams(
                    collective_id=mask, has_side_effects=True, vmem_limit_bytes=56 * 2**20
                ),
                name=f"exchange_{mask}",
            )(occupation, rows, kernel_hat, *consts)

        return run

    result = lax.switch(
        pair_mask[0] - 1, [branch(mask) for mask in range(1, 8)], rows, occupation, kernel_hat, *consts
    )
    return result.reshape(PLANES, 72, 2, 128).transpose(2, 0, 1, 3).reshape(2, PLANES, G * G)


def solution(mesh):
    return jax.shard_map(
        local,
        mesh=mesh,
        in_specs=(P("grp", "slab", None), P("grp"), P("slab", None), P()),
        out_specs=P("grp", "slab", None),
        check_vma=False,
    )
```

```python
import functools
import math

import jax
import jax.numpy as jnp
import ml_dtypes
import numpy as np
from jax import lax
from jax.experimental import pallas as pl
from jax.experimental.pallas import tpu as pltpu
from jax.sharding import PartitionSpec as P

MESH = pl.DeviceIdType.MESH
G = 96
N = 192
PLANES = 6
CHUNKS = 3
SLABS = 16
KZ = 12
F32 = jnp.float32
BF16 = jnp.bfloat16


def halves(table):
    table = np.asarray(table, np.float64)
    high = table.astype(np.float32).astype(ml_dtypes.bfloat16)
    low = (table - high.astype(np.float64)).astype(np.float32).astype(ml_dtypes.bfloat16)
    return np.stack([high, low])


def rotation(freq, place):
    angle = 2.0 * math.pi * ((np.outer(freq, place)) % N) / N
    return np.cos(angle), np.sin(angle)


def tables():
    every = np.arange(N)
    z = np.arange(G)
    y = np.array([4 * q + r for r in range(4) for q in range(24)])
    cos_z, sin_z = rotation(every, z)
    z_both = np.zeros((N, 256))
    z_both[:, :G], z_both[:, 128 : 128 + G] = cos_z, sin_z
    y_fwd = np.zeros((2, G, 2, 2, 128))
    for parity in range(2):
        cos_y, sin_y = rotation(2 * np.arange(G) + parity, y)
        y_fwd[0, :, 0, parity, :G] = cos_y.T
        y_fwd[1, :, 0, parity, :G] = sin_y.T
        y_fwd[0, :, 1, parity, :G] = -sin_y.T
        y_fwd[1, :, 1, parity, :G] = cos_y.T
    x_fwd, x_inv = [], []
    for c in range(CHUNKS):
        cos_x, sin_x = rotation(every, np.array([PLANES * s + 2 * c + k for k in range(2) for s in range(SLABS)]))
        pair = halves(np.block([[cos_x, sin_x], [-sin_x, cos_x]]))
        x_fwd.append(np.concatenate([pair[0], pair[0], pair[1]], axis=1))
        x_inv.append(np.concatenate([pair[0].T, pair[1].T], axis=0))
    return [halves(z_both), halves(y_fwd.reshape(N, 512)), np.stack(x_fwd), np.stack(x_inv)]


STEPS = [(1, 2), (1, 0), (0, 1), (0, 3), (1, 1), (0, 2), (1, 3)]
PEERS = [(y, x, 0) for y, x in STEPS] + [(y, x, 1) for y, x in STEPS] + [(0, 0, 1)]


def split(value):
    high = value.astype(BF16)
    return high, (value - high.astype(F32)).astype(BF16)


def dot(left, right, contract=((1,), (0,))):
    return lax.dot_general(left, right, (contract, ((), ())), preferred_element_type=F32)


def triple(left, right, contract=((1,), (0,))):
    return (
        dot(left[0], right[0], contract)
        + dot(left[0], right[1], contract)
        + dot(left[1], right[0], contract)
    )


def kernel(
    mask,
    occ_ref, orb_in, kern_in, z_in, y_in, x_in, xi_in,
    out,
    orb, kern, z_tab, y_tab, x_tab, xi_tab,
    theirs, weights, their_weights, pencils, send_a, recv_a, send_b, recv_b, spec, gspec, flat, kmat,
    total, high_f, low_f, back, landed,
    in_s, exch_s, exch_r, w_s, w_r, a_s, a_r, b_s, b_r, ret_s, ret_r,
):
    grp = lax.axis_index("grp")
    me = lax.axis_index("slab")
    partner = grp
    for bit in range(3):
        if mask >> bit & 1:
            partner = partner + (1 - 2 * (grp // 2**bit % 2)) * 2**bit
    upper = grp // 2 ** (mask.bit_length() - 1) % 2
    mine_y, mine_x, mine_c = me // 8, me // 2 % 4, me % 2
    peers = [((mine_y + y) % 2 * 4 + (mine_x + x) % 4) * 2 + (mine_c + c) % 2 for y, x, c in PEERS]

    barrier = pltpu.get_barrier_semaphore()
    pl.semaphore_signal(barrier, inc=1, device_id=(partner, me), device_id_type=MESH)
    for peer in peers:
        pl.semaphore_signal(barrier, inc=1, device_id=(grp, peer), device_id_type=MESH)

    stage = [
        pltpu.make_async_copy(source, target, in_s.at[i])
        for i, (source, target) in enumerate(
            (
                (orb_in, orb),
                (kern_in, kern),
                (z_in, z_tab.at[:, pl.ds(0, N), :]),
                (y_in, y_tab.at[:, pl.ds(64, N), :]),
                (x_in, x_tab),
                (xi_in, xi_tab),
            )
        )
    ]
    for copy in stage:
        copy.start()
    own_w0 = occ_ref[0].astype(F32) * 0.25
    own_w1 = occ_ref[1].astype(F32) * 0.25
    weights[0:1, :] = jnp.full((1, 128), own_w0, F32)
    weights[1:2, :] = jnp.full((1, 128), own_w1, F32)
    pencils[...] = jnp.zeros(pencils.shape, F32)
    z_tab[:, N:, :] = jnp.zeros((2, 64, 256), BF16)
    y_tab[:, :64, :] = jnp.zeros((2, 64, 512), BF16)
    y_tab[:, 64 + N :, :] = jnp.zeros((2, 64, 512), BF16)
    stage[0].wait()
    pl.semaphore_wait(barrier, SLABS)

    def exch_copy(c):
        rows = pl.ds(c * 288, 288)
        return pltpu.make_async_remote_copy(
            orb.at[rows], theirs.at[rows], exch_s.at[c], exch_r.at[c], device_id=(partner, me), device_id_type=MESH
        )

    for c in range(CHUNKS):
        exch_copy(c).start()
    weight_copy = pltpu.make_async_remote_copy(
        weights, their_weights, w_s, w_r, device_id=(partner, me), device_id_type=MESH
    )
    weight_copy.start()

    stage[1].wait()

    def flatten(step, carry):
        for sub in range(8):
            m = step * 8 + sub
            flat[pl.ds(m, KZ, stride=288), :] = kern[:, pl.ds(pl.multiple_of(m * 128, 128), 128)] * (1.0 / N**3)
        return carry

    lax.fori_loop(0, 36, flatten, 0)

    def turn(j, carry):
        pad = jnp.zeros((32, 128), F32)
        t0, t1, t2 = [
            jnp.concatenate([flat[pl.ds(j * 288 + l, G, stride=3), :], pad], axis=0).T for l in range(3)
        ]
        base = pl.multiple_of(j * N, N)
        kmat[pl.ds(base, 128), 0:128] = t0
        kmat[pl.ds(base + 128, 64), 0:128] = t1[:64]
        kmat[pl.ds(base, 64), 128:256] = t1[64:]
        kmat[pl.ds(base + 64, 128), 128:256] = t2
        return carry

    lax.fori_loop(0, KZ, turn, 0)
    for copy in stage[2:]:
        copy.wait()

    def orbital(ref, c, which):
        return [ref[pl.ds(c * 288 + 2 * l + which, 48, stride=6), :] for l in range(3)]

    def send_all(sent, landing, s_sem, r_sem, c):
        for peer in peers:
            pltpu.make_async_remote_copy(
                sent.at[pl.ds(c * 576 + peer * 36, 36)],
                landing.at[pl.ds(c * 576 + me * 36, 36)],
                s_sem.at[c],
                r_sem.at[c],
                device_id=(grp, peer),
                device_id_type=MESH,
            ).start()
        rows = pl.ds(c * 576 + me * 36, 36)
        pltpu.make_async_copy(sent.at[rows], landing.at[rows], r_sem.at[c]).start()

    def wait_rows(ref, sem, start, count):
        rows = pl.ds(start, count)
        pltpu.make_async_copy(ref.at[rows], ref.at[rows], sem).wait()

    def forward_z(c, carry):
        exch_copy(c).wait_recv()
        first = jnp.concatenate(
            [a * b for a, b in zip(orbital(orb, c, 0), orbital(theirs, c, upper))], axis=1
        )
        second = jnp.concatenate(
            [a * b for a, b in zip(orbital(orb, c, 1), orbital(theirs, c, 1 - upper))], axis=1
        )
        for r in range(4):
            for k in range(2):
                one = first[24 * k : 24 * k + 24, G * r : G * r + G]
                two = second[24 * k : 24 * k + 24, G * r : G * r + G]
                at = k * N + r * 24
                pencils[at : at + 24, 0:G] = one
                pencils[at : at + 24, 128 : 128 + G] = two
                pencils[at + G : at + G + 24, 0:G] = two
                pencils[at + G : at + G + 24, 128 : 128 + G] = -one
        spread = triple((z_tab[0, :N], z_tab[1, :N]), split(pencils[...]), ((1,), (1,)))
        for l in range(3):
            send_a[pl.ds(c * 576 + l, N, stride=3), :] = spread[:, 128 * l : 128 * l + 128]
        send_all(send_a, recv_a, a_s, a_r, c)
        return carry

    lax.fori_loop(0, CHUNKS, forward_z, 0)

    def forward_y(c):
        wait_rows(recv_a, a_r.at[c], c * 576, 576)
        wire = jnp.concatenate([recv_a[pl.ds(c * 576 + l, N, stride=3), :] for l in range(3)], axis=1)
        high, low = split(wire)
        for k in range(2):
            lanes = slice(128 * k, 128 * k + 256)
            rows = slice(64, 320) if k == 0 else slice(0, 256)
            result = triple((high[:, lanes], low[:, lanes]), (y_tab[0, rows], y_tab[1, rows]))
            for l in range(4):
                spec[pl.ds(l * 384 + k * N, N), :] = result[:, 128 * l : 128 * l + 128]

    def partial_x(j, c):
        field = jnp.concatenate(
            [
                jnp.concatenate(
                    [
                        spec[pl.ds((2 * d + parity) * 384 + k * N + j, SLABS, stride=KZ), :]
                        for d in range(2)
                        for k in range(2)
                    ],
                    axis=0,
                )
                for parity in range(2)
            ],
            axis=1,
        )
        high, low = split(field)
        return dot(x_tab[c], jnp.concatenate([high, low, high], axis=0))

    def block(j):
        return pl.ds(pl.multiple_of(j * 384, 384), 384)

    def inverse_x(c, j, high, low):
        wide = dot(xi_tab[c], high)
        field = wide[:64] + wide[64:] + dot(xi_tab[c, :64], low)
        for parity in range(2):
            for d in range(2):
                for k in range(2):
                    row = (d * 2 + k) * SLABS
                    gspec[pl.ds((2 * d + parity) * 384 + k * N + j, SLABS, stride=KZ), :] = field[
                        row : row + SLABS, 128 * parity : 128 * parity + 128
                    ]

    def begin(j, carry):
        total[block(j), :] = partial_x(j, 0)
        return carry

    def add(j, carry):
        total[block(j), :] = total[block(j), :] + partial_x(j, 1)
        return carry

    def turn_back(j, carry):
        value = total[block(j), :] + partial_x(j, 2)
        weight = kmat[pl.ds(pl.multiple_of(j * N, N), N), :]
        high, low = split(jnp.concatenate([value[:N] * weight, value[N:] * weight], axis=0))
        high_f[block(j), :] = high
        low_f[block(j), :] = low
        inverse_x(0, j, high, low)
        return carry

    for c, step in enumerate((begin, add, turn_back)):
        forward_y(c)
        lax.fori_loop(0, KZ, step, 0)

    def inverse_y(c, carry):
        @pl.when(c > 0)
        def _():
            def back_x(j, carry):
                inverse_x(c, j, high_f[block(j), :], low_f[block(j), :])
                return carry

            lax.fori_loop(0, KZ, back_x, 0)

        parts = []
        for k in range(2):
            wide = jnp.concatenate([gspec[pl.ds(l * 384 + k * N, N), :] for l in range(4)], axis=1)
            rows = slice(64, 320) if k == 0 else slice(0, 256)
            parts.append(triple(split(wide), (y_tab[0, rows], y_tab[1, rows]), ((1,), (1,))))
        tiles = [parts[0][:, :128], parts[0][:, 128:] + parts[1][:, :128], parts[1][:, 128:]]
        for l in range(3):
            send_b[pl.ds(c * 576 + l, N, stride=3), :] = tiles[l]
        send_all(send_b, recv_b, b_s, b_r, c)
        return carry

    lax.fori_loop(0, CHUNKS, inverse_y, 0)
    weight_copy.wait_recv()

    def ret_copy(c):
        rows = pl.ds(c * 288, 288)
        return pltpu.make_async_remote_copy(
            back.at[rows], landed.at[rows], ret_s.at[c], ret_r.at[c], device_id=(partner, me), device_id_type=MESH
        )

    def inverse_z(c, carry):
        wait_rows(recv_b, b_r.at[c], c * 576, 576)
        pad = jnp.zeros((64, 128), F32)
        turned = jnp.concatenate(
            [
                jnp.concatenate([recv_b[pl.ds(c * 576 + l, N, stride=3), :], pad], axis=0).T
                for l in range(3)
            ],
            axis=0,
        )
        both = triple(split(turned), (z_tab[0], z_tab[1]))
        first, second = [], []
        for r in range(4):
            ones, twos = [], []
            for k in range(2):
                at = k * N + r * 24
                re = both[at : at + 24]
                im = both[at + G : at + G + 24]
                ones.append(re[:, :G] - im[:, 128 : 128 + G])
                twos.append(re[:, 128 : 128 + G] + im[:, :G])
            first.append(jnp.concatenate(ones, axis=0))
            second.append(jnp.concatenate(twos, axis=0))
        first = jnp.concatenate(first, axis=1)
        second = jnp.concatenate(second, axis=1)
        w_first = their_weights[pl.ds(upper, 1), :]
        w_second = their_weights[pl.ds(1 - upper, 1), :]
        for field, which, other, near, far in (
            (first, 0, upper, own_w0, w_first),
            (second, 1, 1 - upper, own_w1, w_second),
        ):
            mine, partners = orbital(orb, c, which), orbital(theirs, c, other)
            for l in range(3):
                tile = field[:, 128 * l : 128 * l + 128]
                out[pl.ds(c * 288 + 2 * l + which, 48, stride=6), :] = -(far * tile * partners[l])
                back[pl.ds(c * 288 + 2 * l + other, 48, stride=6), :] = -(near * tile * mine[l])
        ret_copy(c).start()
        return carry

    lax.fori_loop(0, CHUNKS, inverse_z, 0)

    def finish(c, carry):
        ret_copy(c).wait_recv()
        rows = pl.ds(pl.multiple_of(c * 288, 288), 288)
        out[rows, :] = out[rows, :] + landed[rows, :]
        return carry

    lax.fori_loop(0, CHUNKS, finish, 0)

    weight_copy.wait_send()
    for c in range(CHUNKS):
        exch_copy(c).wait_send()
        ret_copy(c).wait_send()
        wait_rows(send_a, a_s.at[c], 0, 540)
        wait_rows(send_b, b_s.at[c], 0, 540)


def local(orbitals, occupation, kernel_hat, pair_mask):
    rows = orbitals.reshape(2, PLANES, 72, 128).transpose(1, 2, 0, 3).reshape(864, 128)
    consts = [jnp.asarray(value) for value in tables()]
    dma = pltpu.SemaphoreType.DMA

    def branch(mask):
        def run(rows, occupation, kernel_hat, *consts):
            return pl.pallas_call(
                functools.partial(kernel, mask),
                out_shape=jax.ShapeDtypeStruct((864, 128), F32),
                in_specs=[pl.BlockSpec(memory_space=pltpu.SMEM)] + [pl.BlockSpec(memory_space=pl.ANY)] * 6,
                out_specs=pl.BlockSpec(memory_space=pltpu.VMEM),
                scratch_shapes=[
                    pltpu.VMEM((864, 128), F32),
                    pltpu.VMEM((KZ, N * N), F32),
                    pltpu.VMEM((2, 256, 256), BF16),
                    pltpu.VMEM((2, 320, 512), BF16),
                    pltpu.VMEM((CHUNKS, 384, N), BF16),
                    pltpu.VMEM((CHUNKS, 128, 384), BF16),
                    pltpu.VMEM((864, 128), F32),
                    pltpu.VMEM((8, 128), F32),
                    pltpu.VMEM((8, 128), F32),
                    pltpu.VMEM((384, 256), F32),
                    pltpu.VMEM((1728, 128), F32),
                    pltpu.VMEM((1728, 128), F32),
                    pltpu.VMEM((1728, 128), F32),
                    pltpu.VMEM((1728, 128), F32),
                    pltpu.VMEM((1536, 128), F32),
                    pltpu.VMEM((1536, 128), F32),
                    pltpu.VMEM((KZ * 288, 128), F32),
                    pltpu.VMEM((KZ * N, 256), F32),
                    pltpu.VMEM((KZ * 384, 256), F32),
                    pltpu.VMEM((KZ * 384, 256), BF16),
                    pltpu.VMEM((KZ * 384, 256), BF16),
                    pltpu.VMEM((864, 128), F32),
                    pltpu.VMEM((864, 128), F32),
                    dma((6,)), dma((CHUNKS,)), dma((CHUNKS,)), dma, dma,
                    dma((CHUNKS,)), dma((CHUNKS,)), dma((CHUNKS,)), dma((CHUNKS,)),
                    dma((CHUNKS,)), dma((CHUNKS,)),
                ],
                compiler_params=pltpu.CompilerParams(
                    collective_id=mask, has_side_effects=True, vmem_limit_bytes=56 * 2**20
                ),
                name=f"exchange_{mask}",
            )(occupation, rows, kernel_hat, *consts)

        return run

    result = lax.switch(
        pair_mask[0] - 1, [branch(mask) for mask in range(1, 8)], rows, occupation, kernel_hat, *consts
    )
    return result.reshape(PLANES, 72, 2, 128).transpose(2, 0, 1, 3).reshape(2, PLANES, G * G)


def solution(mesh):
    return jax.shard_map(
        local,
        mesh=mesh,
        in_specs=(P("grp", "slab", None), P("grp"), P("slab", None), P()),
        out_specs=P("grp", "slab", None),
        check_vma=False,
    )
```

```python
import functools
import math

import jax
import jax.numpy as jnp
import ml_dtypes
import numpy as np
from jax import lax
from jax.experimental import pallas as pl
from jax.experimental.layout import Layout, with_layout_constraint
from jax.experimental.pallas import tpu as pltpu
from jax.sharding import PartitionSpec as P

MESH = pl.DeviceIdType.MESH
G = 96
N = 192
PLANES = 6
CHUNKS = 3
SLABS = 16
KZ = 12
F32 = jnp.float32
BF16 = jnp.bfloat16


def halves(table):
    table = np.asarray(table, np.float64)
    high = table.astype(np.float32).astype(ml_dtypes.bfloat16)
    low = (table - high.astype(np.float64)).astype(np.float32).astype(ml_dtypes.bfloat16)
    return np.stack([high, low])


def rotation(freq, place):
    angle = 2.0 * math.pi * ((np.outer(freq, place)) % N) / N
    return np.cos(angle), np.sin(angle)


def tables():
    every = np.arange(N)
    z = np.arange(G)
    y = np.array([4 * q + r for r in range(4) for q in range(24)])
    cos_z, sin_z = rotation(every, z)
    z_both = np.zeros((N, 256))
    z_both[:, :G], z_both[:, 128 : 128 + G] = cos_z, sin_z
    y_fwd = np.zeros((2, G, 2, 2, 128))
    for parity in range(2):
        cos_y, sin_y = rotation(2 * np.arange(G) + parity, y)
        y_fwd[0, :, 0, parity, :G] = cos_y.T
        y_fwd[1, :, 0, parity, :G] = sin_y.T
        y_fwd[0, :, 1, parity, :G] = -sin_y.T
        y_fwd[1, :, 1, parity, :G] = cos_y.T
    x_fwd, x_inv = [], []
    for c in range(CHUNKS):
        cos_x, sin_x = rotation(every, np.array([PLANES * s + 2 * c + k for k in range(2) for s in range(SLABS)]))
        pair = halves(np.block([[cos_x, sin_x], [-sin_x, cos_x]]))
        x_fwd.append(np.concatenate([pair[0], pair[0], pair[1]], axis=1))
        x_inv.append(np.concatenate([pair[0].T, pair[1].T], axis=0))
    return [halves(z_both), halves(y_fwd.reshape(N, 512)), np.stack(x_fwd), np.stack(x_inv)]


STEPS = [(1, 2), (1, 0), (0, 1), (0, 3), (1, 1), (0, 2), (1, 3)]
PEERS = [(y, x, 0) for y, x in STEPS] + [(y, x, 1) for y, x in STEPS] + [(0, 0, 1)]


def split(value):
    high = value.astype(BF16)
    return high, (value - high.astype(F32)).astype(BF16)


def dot(left, right, contract=((1,), (0,))):
    return lax.dot_general(left, right, (contract, ((), ())), preferred_element_type=F32)


def triple(left, right, contract=((1,), (0,))):
    return (
        dot(left[0], right[0], contract)
        + dot(left[0], right[1], contract)
        + dot(left[1], right[0], contract)
    )


def kernel(
    mask,
    occ_ref, orb_in, kern_in, z_in, y_in, x_in, xi_in,
    out,
    orb, kern, z_tab, y_tab, x_tab, xi_tab,
    theirs, weights, their_weights, pencils, send_a, recv_a, send_b, recv_b, spec, gspec, flat, kmat,
    total, high_f, low_f, back, landed,
    in_s, exch_s, exch_r, w_s, w_r, a_s, a_r, b_s, b_r, ret_s, ret_r,
):
    grp = lax.axis_index("grp")
    me = lax.axis_index("slab")
    partner = grp
    for bit in range(3):
        if mask >> bit & 1:
            partner = partner + (1 - 2 * (grp // 2**bit % 2)) * 2**bit
    upper = grp // 2 ** (mask.bit_length() - 1) % 2
    mine_y, mine_x, mine_c = me // 8, me // 2 % 4, me % 2
    peers = [((mine_y + y) % 2 * 4 + (mine_x + x) % 4) * 2 + (mine_c + c) % 2 for y, x, c in PEERS]

    barrier = pltpu.get_barrier_semaphore()
    pl.semaphore_signal(barrier, inc=1, device_id=(partner, me), device_id_type=MESH)
    for peer in peers:
        pl.semaphore_signal(barrier, inc=1, device_id=(grp, peer), device_id_type=MESH)

    stage = [
        pltpu.make_async_copy(source, target, in_s.at[i])
        for i, (source, target) in enumerate(
            (
                (orb_in, orb),
                (kern_in, kern),
                (z_in, z_tab.at[:, pl.ds(0, N), :]),
                (y_in, y_tab.at[:, pl.ds(64, N), :]),
                (x_in, x_tab),
                (xi_in, xi_tab),
            )
        )
    ]
    for copy in stage:
        copy.start()
    own_w0 = occ_ref[0].astype(F32) * 0.25
    own_w1 = occ_ref[1].astype(F32) * 0.25
    weights[0:1, :] = jnp.full((1, 128), own_w0, F32)
    weights[1:2, :] = jnp.full((1, 128), own_w1, F32)
    pencils[...] = jnp.zeros(pencils.shape, F32)
    z_tab[:, N:, :] = jnp.zeros((2, 64, 256), BF16)
    y_tab[:, :64, :] = jnp.zeros((2, 64, 512), BF16)
    y_tab[:, 64 + N :, :] = jnp.zeros((2, 64, 512), BF16)
    stage[0].wait()
    pl.semaphore_wait(barrier, SLABS)

    def exch_copy(c):
        rows = pl.ds(c * 288, 288)
        return pltpu.make_async_remote_copy(
            orb.at[rows], theirs.at[rows], exch_s.at[c], exch_r.at[c], device_id=(partner, me), device_id_type=MESH
        )

    for c in range(CHUNKS):
        exch_copy(c).start()
    weight_copy = pltpu.make_async_remote_copy(
        weights, their_weights, w_s, w_r, device_id=(partner, me), device_id_type=MESH
    )
    weight_copy.start()

    stage[1].wait()

    def flatten(step, carry):
        for sub in range(8):
            m = step * 8 + sub
            flat[pl.ds(m, KZ, stride=288), :] = kern[:, pl.ds(pl.multiple_of(m * 128, 128), 128)] * (1.0 / N**3)
        return carry

    lax.fori_loop(0, 36, flatten, 0)

    def turn(j, carry):
        pad = jnp.zeros((32, 128), F32)
        t0, t1, t2 = [
            jnp.concatenate([flat[pl.ds(j * 288 + l, G, stride=3), :], pad], axis=0).T for l in range(3)
        ]
        base = pl.multiple_of(j * N, N)
        kmat[pl.ds(base, 128), 0:128] = t0
        kmat[pl.ds(base + 128, 64), 0:128] = t1[:64]
        kmat[pl.ds(base, 64), 128:256] = t1[64:]
        kmat[pl.ds(base + 64, 128), 128:256] = t2
        return carry

    lax.fori_loop(0, KZ, turn, 0)
    for copy in stage[2:]:
        copy.wait()

    def orbital(ref, c, which):
        return [ref[pl.ds(c * 288 + 2 * l + which, 48, stride=6), :] for l in range(3)]

    def send_all(sent, landing, s_sem, r_sem, c):
        for peer in peers:
            pltpu.make_async_remote_copy(
                sent.at[pl.ds(c * 576 + peer * 36, 36)],
                landing.at[pl.ds(c * 576 + me * 36, 36)],
                s_sem.at[c],
                r_sem.at[c],
                device_id=(grp, peer),
                device_id_type=MESH,
            ).start()
        rows = pl.ds(c * 576 + me * 36, 36)
        pltpu.make_async_copy(sent.at[rows], landing.at[rows], r_sem.at[c]).start()

    def wait_rows(ref, sem, start, count):
        rows = pl.ds(start, count)
        pltpu.make_async_copy(ref.at[rows], ref.at[rows], sem).wait()

    def forward_z(c, carry):
        exch_copy(c).wait_recv()
        first = jnp.concatenate(
            [a * b for a, b in zip(orbital(orb, c, 0), orbital(theirs, c, upper))], axis=1
        )
        second = jnp.concatenate(
            [a * b for a, b in zip(orbital(orb, c, 1), orbital(theirs, c, 1 - upper))], axis=1
        )
        for r in range(4):
            for k in range(2):
                one = first[24 * k : 24 * k + 24, G * r : G * r + G]
                two = second[24 * k : 24 * k + 24, G * r : G * r + G]
                at = k * N + r * 24
                pencils[at : at + 24, 0:G] = one
                pencils[at : at + 24, 128 : 128 + G] = two
                pencils[at + G : at + G + 24, 0:G] = two
                pencils[at + G : at + G + 24, 128 : 128 + G] = -one
        spread = triple((z_tab[0, :N], z_tab[1, :N]), split(pencils[...]), ((1,), (1,)))
        for l in range(3):
            send_a[pl.ds(c * 576 + l, N, stride=3), :] = spread[:, 128 * l : 128 * l + 128]
        send_all(send_a, recv_a, a_s, a_r, c)
        return carry

    lax.fori_loop(0, CHUNKS, forward_z, 0)

    def forward_y(c):
        wait_rows(recv_a, a_r.at[c], c * 576, 576)
        wire = jnp.concatenate([recv_a[pl.ds(c * 576 + l, N, stride=3), :] for l in range(3)], axis=1)
        high, low = split(wire)
        for k in range(2):
            lanes = slice(128 * k, 128 * k + 256)
            rows = slice(64, 320) if k == 0 else slice(0, 256)
            result = triple((high[:, lanes], low[:, lanes]), (y_tab[0, rows], y_tab[1, rows]))
            for l in range(4):
                spec[pl.ds(l * 384 + k * N, N), :] = result[:, 128 * l : 128 * l + 128]

    def partial_x(j, c):
        field = jnp.concatenate(
            [
                jnp.concatenate(
                    [
                        spec[pl.ds((2 * d + parity) * 384 + k * N + j, SLABS, stride=KZ), :]
                        for d in range(2)
                        for k in range(2)
                    ],
                    axis=0,
                )
                for parity in range(2)
            ],
            axis=1,
        )
        high, low = split(field)
        return dot(x_tab[c], jnp.concatenate([high, low, high], axis=0))

    def block(j):
        return pl.ds(pl.multiple_of(j * 384, 384), 384)

    def inverse_x(c, j, high, low):
        wide = dot(xi_tab[c], high)
        field = wide[:64] + wide[64:] + dot(xi_tab[c, :64], low)
        for parity in range(2):
            for d in range(2):
                for k in range(2):
                    row = (d * 2 + k) * SLABS
                    gspec[pl.ds((2 * d + parity) * 384 + k * N + j, SLABS, stride=KZ), :] = field[
                        row : row + SLABS, 128 * parity : 128 * parity + 128
                    ]

    def begin(j, carry):
        total[block(j), :] = partial_x(j, 0)
        return carry

    def add(j, carry):
        total[block(j), :] = total[block(j), :] + partial_x(j, 1)
        return carry

    def turn_back(j, carry):
        value = total[block(j), :] + partial_x(j, 2)
        weight = kmat[pl.ds(pl.multiple_of(j * N, N), N), :]
        high, low = split(jnp.concatenate([value[:N] * weight, value[N:] * weight], axis=0))
        high_f[block(j), :] = high
        low_f[block(j), :] = low
        inverse_x(0, j, high, low)
        return carry

    for c, step in enumerate((begin, add, turn_back)):
        forward_y(c)
        lax.fori_loop(0, KZ, step, 0, unroll=2 if c == 2 else 1)

    def inverse_y(c, carry):
        @pl.when(c > 0)
        def _():
            def back_x(j, carry):
                inverse_x(c, j, high_f[block(j), :], low_f[block(j), :])
                return carry

            lax.fori_loop(0, KZ, back_x, 0)

        parts = []
        for k in range(2):
            wide = jnp.concatenate([gspec[pl.ds(l * 384 + k * N, N), :] for l in range(4)], axis=1)
            rows = slice(64, 320) if k == 0 else slice(0, 256)
            parts.append(triple(split(wide), (y_tab[0, rows], y_tab[1, rows]), ((1,), (1,))))
        tiles = [parts[0][:, :128], parts[0][:, 128:] + parts[1][:, :128], parts[1][:, 128:]]
        for l in range(3):
            send_b[pl.ds(c * 576 + l, N, stride=3), :] = tiles[l]
        send_all(send_b, recv_b, b_s, b_r, c)
        return carry

    lax.fori_loop(0, CHUNKS, inverse_y, 0)
    weight_copy.wait_recv()

    def ret_copy(c):
        rows = pl.ds(c * 288, 288)
        return pltpu.make_async_remote_copy(
            back.at[rows], landed.at[rows], ret_s.at[c], ret_r.at[c], device_id=(partner, me), device_id_type=MESH
        )

    def inverse_z(c, carry):
        wait_rows(recv_b, b_r.at[c], c * 576, 576)
        pad = jnp.zeros((64, 128), F32)
        turned = jnp.concatenate(
            [
                jnp.concatenate([recv_b[pl.ds(c * 576 + l, N, stride=3), :], pad], axis=0).T
                for l in range(3)
            ],
            axis=0,
        )
        both = triple(split(turned), (z_tab[0], z_tab[1]))
        first, second = [], []
        for r in range(4):
            ones, twos = [], []
            for k in range(2):
                at = k * N + r * 24
                re = both[at : at + 24]
                im = both[at + G : at + G + 24]
                ones.append(re[:, :G] - im[:, 128 : 128 + G])
                twos.append(re[:, 128 : 128 + G] + im[:, :G])
            first.append(jnp.concatenate(ones, axis=0))
            second.append(jnp.concatenate(twos, axis=0))
        first = jnp.concatenate(first, axis=1)
        second = jnp.concatenate(second, axis=1)
        w_first = their_weights[pl.ds(upper, 1), :]
        w_second = their_weights[pl.ds(1 - upper, 1), :]
        for field, which, other, near, far in (
            (first, 0, upper, own_w0, w_first),
            (second, 1, 1 - upper, own_w1, w_second),
        ):
            mine, partners = orbital(orb, c, which), orbital(theirs, c, other)
            for l in range(3):
                tile = field[:, 128 * l : 128 * l + 128]
                out[pl.ds(c * 288 + 2 * l + which, 48, stride=6), :] = -(far * tile * partners[l])
                back[pl.ds(c * 288 + 2 * l + other, 48, stride=6), :] = -(near * tile * mine[l])
        ret_copy(c).start()
        return carry

    lax.fori_loop(0, CHUNKS, inverse_z, 0)

    def finish(c, carry):
        ret_copy(c).wait_recv()
        rows = pl.ds(pl.multiple_of(c * 288, 288), 288)
        out[rows, :] = out[rows, :] + landed[rows, :]
        return carry

    lax.fori_loop(0, CHUNKS, finish, 0)

    weight_copy.wait_send()
    for c in range(CHUNKS):
        exch_copy(c).wait_send()
        ret_copy(c).wait_send()
        wait_rows(send_a, a_s.at[c], 0, 540)
        wait_rows(send_b, b_s.at[c], 0, 540)


def local(orbitals, occupation, kernel_hat, pair_mask):
    rows = orbitals.reshape(2, PLANES, 72, 128).transpose(1, 2, 0, 3).reshape(864, 128)
    consts = [jnp.asarray(value) for value in tables()]
    dma = pltpu.SemaphoreType.DMA

    def branch(mask):
        def run(rows, occupation, kernel_hat, *consts):
            return pl.pallas_call(
                functools.partial(kernel, mask),
                out_shape=jax.ShapeDtypeStruct((864, 128), F32),
                in_specs=[pl.BlockSpec(memory_space=pltpu.SMEM)] + [pl.BlockSpec(memory_space=pl.ANY)] * 6,
                out_specs=pl.BlockSpec(memory_space=pltpu.VMEM),
                scratch_shapes=[
                    pltpu.VMEM((864, 128), F32),
                    pltpu.VMEM((KZ, N * N), F32),
                    pltpu.VMEM((2, 256, 256), BF16),
                    pltpu.VMEM((2, 320, 512), BF16),
                    pltpu.VMEM((CHUNKS, 384, N), BF16),
                    pltpu.VMEM((CHUNKS, 128, 384), BF16),
                    pltpu.VMEM((864, 128), F32),
                    pltpu.VMEM((8, 128), F32),
                    pltpu.VMEM((8, 128), F32),
                    pltpu.VMEM((384, 256), F32),
                    pltpu.VMEM((1728, 128), F32),
                    pltpu.VMEM((1728, 128), F32),
                    pltpu.VMEM((1728, 128), F32),
                    pltpu.VMEM((1728, 128), F32),
                    pltpu.VMEM((1536, 128), F32),
                    pltpu.VMEM((1536, 128), F32),
                    pltpu.VMEM((KZ * 288, 128), F32),
                    pltpu.VMEM((KZ * N, 256), F32),
                    pltpu.VMEM((KZ * 384, 256), F32),
                    pltpu.VMEM((KZ * 384, 256), BF16),
                    pltpu.VMEM((KZ * 384, 256), BF16),
                    pltpu.VMEM((864, 128), F32),
                    pltpu.VMEM((864, 128), F32),
                    dma((6,)), dma((CHUNKS,)), dma((CHUNKS,)), dma, dma,
                    dma((CHUNKS,)), dma((CHUNKS,)), dma((CHUNKS,)), dma((CHUNKS,)),
                    dma((CHUNKS,)), dma((CHUNKS,)),
                ],
                compiler_params=pltpu.CompilerParams(
                    collective_id=mask, has_side_effects=True, vmem_limit_bytes=56 * 2**20
                ),
                name=f"exchange_{mask}",
            )(occupation, rows, kernel_hat, *consts)

        return run

    result = lax.switch(
        pair_mask[0] - 1, [branch(mask) for mask in range(1, 8)], rows, occupation, kernel_hat, *consts
    )
    planes = result.reshape(PLANES, 72, 2, 128).transpose(2, 0, 1, 3)
    planes = with_layout_constraint(planes, Layout((1, 2, 0, 3)))
    return planes.reshape(2, PLANES, G * G)


def solution(mesh):
    return jax.shard_map(
        local,
        mesh=mesh,
        in_specs=(P("grp", "slab", None), P("grp"), P("slab", None), P()),
        out_specs=P("grp", "slab", None),
        check_vma=False,
    )
```

```python
import functools
import math

import jax
import jax.numpy as jnp
import ml_dtypes
import numpy as np
from jax import lax
from jax.experimental import pallas as pl
from jax.experimental.layout import Layout, with_layout_constraint
from jax.experimental.pallas import tpu as pltpu
from jax.sharding import PartitionSpec as P

MESH = pl.DeviceIdType.MESH
G = 96
N = 192
PLANES = 6
CHUNKS = 3
SLABS = 16
KZ = 12
F32 = jnp.float32
BF16 = jnp.bfloat16


def halves(table):
    table = np.asarray(table, np.float64)
    high = table.astype(np.float32).astype(ml_dtypes.bfloat16)
    low = (table - high.astype(np.float64)).astype(np.float32).astype(ml_dtypes.bfloat16)
    return np.stack([high, low])


def rotation(freq, place):
    angle = 2.0 * math.pi * ((np.outer(freq, place)) % N) / N
    return np.cos(angle), np.sin(angle)


def tables():
    every = np.arange(N)
    z = np.arange(G)
    y = np.array([4 * q + r for r in range(4) for q in range(24)])
    cos_z, sin_z = rotation(every, z)
    z_both = np.zeros((N, 256))
    z_both[:, :G], z_both[:, 128 : 128 + G] = cos_z, sin_z
    y_fwd = np.zeros((2, G, 2, 2, 128))
    for parity in range(2):
        cos_y, sin_y = rotation(2 * np.arange(G) + parity, y)
        y_fwd[0, :, 0, parity, :G] = cos_y.T
        y_fwd[1, :, 0, parity, :G] = sin_y.T
        y_fwd[0, :, 1, parity, :G] = -sin_y.T
        y_fwd[1, :, 1, parity, :G] = cos_y.T
    x_fwd, x_inv = [], []
    for c in range(CHUNKS):
        cos_x, sin_x = rotation(every, np.array([PLANES * s + 2 * c + k for k in range(2) for s in range(SLABS)]))
        pair = halves(np.block([[cos_x, sin_x], [-sin_x, cos_x]]))
        x_fwd.append(np.concatenate([pair[0], pair[0], pair[1]], axis=1))
        x_inv.append(np.concatenate([pair[0].T, pair[1].T], axis=0))
    return [halves(z_both), halves(y_fwd.reshape(N, 512)), np.stack(x_fwd), np.stack(x_inv)]


STEPS = [(1, 2), (1, 0), (0, 1), (0, 3), (1, 1), (0, 2), (1, 3)]
PEERS = [(y, x, 0) for y, x in STEPS] + [(y, x, 1) for y, x in STEPS] + [(0, 0, 1)]


def split(value):
    high = value.astype(BF16)
    return high, (value - high.astype(F32)).astype(BF16)


def dot(left, right, contract=((1,), (0,))):
    return lax.dot_general(left, right, (contract, ((), ())), preferred_element_type=F32)


def triple(left, right, contract=((1,), (0,))):
    return (
        dot(left[0], right[0], contract)
        + dot(left[0], right[1], contract)
        + dot(left[1], right[0], contract)
    )


def kernel(
    mask,
    occ_ref, orb_in, kern_in, z_in, y_in, x_in, xi_in,
    out,
    orb, kern, z_tab, z_back, y_tab, x_tab, xi_tab,
    theirs, weights, their_weights, pencils, pencils_other, send_a, recv_a, send_b, recv_b, spec, gspec, flat, kmat,
    total, high_f, low_f, back, landed,
    in_s, exch_s, exch_r, w_s, w_r, a_s, a_r, b_s, b_r, ret_s, ret_r,
):
    grp = lax.axis_index("grp")
    me = lax.axis_index("slab")
    partner = grp
    for bit in range(3):
        if mask >> bit & 1:
            partner = partner + (1 - 2 * (grp // 2**bit % 2)) * 2**bit
    upper = grp // 2 ** (mask.bit_length() - 1) % 2
    mine_y, mine_x, mine_c = me // 8, me // 2 % 4, me % 2
    peers = [((mine_y + y) % 2 * 4 + (mine_x + x) % 4) * 2 + (mine_c + c) % 2 for y, x, c in PEERS]
    crossing = mask & 1
    groups = [partner if crossing and y and (c or mask == 1) else grp for y, _, c in PEERS]

    barrier = pltpu.get_barrier_semaphore()
    pl.semaphore_signal(barrier, inc=1, device_id=(partner, me), device_id_type=MESH)
    for group, peer in zip(groups, peers):
        pl.semaphore_signal(barrier, inc=1, device_id=(group, peer), device_id_type=MESH)

    stage = [
        pltpu.make_async_copy(source, target, in_s.at[i])
        for i, (source, target) in enumerate(
            (
                (orb_in, orb),
                (kern_in, kern),
                (z_in, z_tab.at[:, pl.ds(0, N), :]),
                (y_in, y_tab.at[:, pl.ds(64, N), :]),
                (x_in, x_tab),
                (xi_in, xi_tab),
            )
        )
    ]
    for copy in stage:
        copy.start()
    own_w0 = occ_ref[0].astype(F32) * 0.25
    own_w1 = occ_ref[1].astype(F32) * 0.25
    weights[0:1, :] = jnp.full((1, 128), own_w0, F32)
    weights[1:2, :] = jnp.full((1, 128), own_w1, F32)
    pencils[...] = jnp.zeros(pencils.shape, F32)
    pencils_other[...] = jnp.zeros(pencils.shape, F32)
    total[...] = jnp.zeros(total.shape, F32)
    z_tab[:, N:, :] = jnp.zeros((2, 64, 256), BF16)
    y_tab[:, :64, :] = jnp.zeros((2, 64, 512), BF16)
    y_tab[:, 64 + N :, :] = jnp.zeros((2, 64, 512), BF16)
    stage[0].wait()
    pl.semaphore_wait(barrier, SLABS)

    def exch_copy(c):
        rows = pl.ds(c * 288, 288)
        return pltpu.make_async_remote_copy(
            orb.at[rows], theirs.at[rows], exch_s.at[c], exch_r.at[c], device_id=(partner, me), device_id_type=MESH
        )

    for c in range(CHUNKS):
        exch_copy(c).start()
    weight_copy = pltpu.make_async_remote_copy(
        weights, their_weights, w_s, w_r, device_id=(partner, me), device_id_type=MESH
    )
    weight_copy.start()

    stage[1].wait()

    def flatten(step, carry):
        for sub in range(8):
            m = step * 8 + sub
            flat[pl.ds(m, KZ, stride=288), :] = kern[:, pl.ds(pl.multiple_of(m * 128, 128), 128)] * (1.0 / N**3)
        return carry

    lax.fori_loop(0, 36, flatten, 0)

    def turn(j, carry):
        pad = jnp.zeros((32, 128), F32)
        t0, t1, t2 = [
            jnp.concatenate([flat[pl.ds(j * 288 + l, G, stride=3), :], pad], axis=0).T for l in range(3)
        ]
        base = pl.multiple_of(j * N, N)
        kmat[pl.ds(base, 128), 0:128] = t0
        kmat[pl.ds(base + 128, 64), 0:128] = t1[:64]
        kmat[pl.ds(base, 64), 128:256] = t1[64:]
        kmat[pl.ds(base + 64, 128), 128:256] = t2
        return carry

    lax.fori_loop(0, KZ, turn, 0)
    for copy in stage[2:]:
        copy.wait()
    if crossing:
        row = lax.broadcasted_iota(jnp.int32, (256, 256), 0)
        away = jnp.abs(row // G - mine_y)
        if mask > 1:
            away = away * jnp.abs(row // KZ % 2 - mine_c)
        other = jnp.minimum(away, 1).astype(F32)
        for part in range(2):
            both = z_tab[part].astype(F32)
            z_back[part, :, 0:256] = (both * (1.0 - other)).astype(BF16)
            z_back[part, :, 256:512] = (both * other).astype(BF16)

    def orbital(ref, c, which):
        return [ref[pl.ds(c * 288 + 2 * l + which, 48, stride=6), :] for l in range(3)]

    def send_all(sent, landing, s_sem, r_sem, c):
        for group, peer in zip(groups, peers):
            pltpu.make_async_remote_copy(
                sent.at[pl.ds(c * 576 + peer * 36, 36)],
                landing.at[pl.ds(c * 576 + me * 36, 36)],
                s_sem.at[c],
                r_sem.at[c],
                device_id=(group, peer),
                device_id_type=MESH,
            ).start()
        rows = pl.ds(c * 576 + me * 36, 36)
        pltpu.make_async_copy(sent.at[rows], landing.at[rows], r_sem.at[c]).start()

    def wait_rows(ref, sem, start, count):
        rows = pl.ds(start, count)
        pltpu.make_async_copy(ref.at[rows], ref.at[rows], sem).wait()

    def pack(ref, left, right):
        first = jnp.concatenate([a * b for a, b in zip(left[0], right[0])], axis=1)
        second = jnp.concatenate([a * b for a, b in zip(left[1], right[1])], axis=1)
        for r in range(4):
            for k in range(2):
                one = first[24 * k : 24 * k + 24, G * r : G * r + G]
                two = second[24 * k : 24 * k + 24, G * r : G * r + G]
                at = k * N + r * 24
                ref[at : at + 24, 0:G] = one
                ref[at : at + 24, 128 : 128 + G] = two
                ref[at + G : at + G + 24, 0:G] = two
                ref[at + G : at + G + 24, 128 : 128 + G] = -one
        return split(ref[...])

    def forward_z(c, carry):
        exch_copy(c).wait_recv()
        own = pack(
            pencils,
            (orbital(orb, c, 0), orbital(orb, c, 1)),
            (orbital(theirs, c, upper), orbital(theirs, c, 1 - upper)),
        )
        if crossing:
            far = pack(
                pencils_other,
                (orbital(theirs, c, 0), orbital(theirs, c, 1)),
                (orbital(orb, c, 1 - upper), orbital(orb, c, upper)),
            )

        def spread(half, field):
            rows = pl.ds(pl.multiple_of(half * G, G), G)
            return triple((z_tab[0, rows], z_tab[1, rows]), field, ((1,), (1,)))

        near_half = spread(mine_y, own)
        if mask == 1:
            far_half = spread(1 - mine_y, far)
        elif crossing:
            same = lax.broadcasted_iota(jnp.int32, (G, 384), 0) // KZ % 2 == mine_c
            far_half = jnp.where(same, spread(1 - mine_y, own), spread(1 - mine_y, far))
        else:
            far_half = spread(1 - mine_y, own)
        for half, value in ((mine_y, near_half), (1 - mine_y, far_half)):
            for l in range(3):
                send_a[pl.ds(c * 576 + half * 288 + l, G, stride=3), :] = value[:, 128 * l : 128 * l + 128]
        send_all(send_a, recv_a, a_s, a_r, c)
        return carry

    lax.fori_loop(0, CHUNKS, forward_z, 0)

    def forward_y(c):
        wait_rows(recv_a, a_r.at[c], c * 576, 576)
        wire = jnp.concatenate([recv_a[pl.ds(c * 576 + l, N, stride=3), :] for l in range(3)], axis=1)
        high, low = split(wire)
        for k in range(2):
            lanes = slice(128 * k, 128 * k + 256)
            rows = slice(64, 320) if k == 0 else slice(0, 256)
            result = triple((high[:, lanes], low[:, lanes]), (y_tab[0, rows], y_tab[1, rows]))
            for l in range(4):
                spec[pl.ds(l * 384 + k * N, N), :] = result[:, 128 * l : 128 * l + 128]

    def partial_x(j, c):
        field = jnp.concatenate(
            [
                jnp.concatenate(
                    [
                        spec[pl.ds((2 * d + parity) * 384 + k * N + j, SLABS, stride=KZ), :]
                        for d in range(2)
                        for k in range(2)
                    ],
                    axis=0,
                )
                for parity in range(2)
            ],
            axis=1,
        )
        high, low = split(field)
        return dot(x_tab[c], jnp.concatenate([high, low, high], axis=0))

    def block(j):
        return pl.ds(pl.multiple_of(j * 384, 384), 384)

    def inverse_x(c, j, high, low):
        wide = dot(xi_tab[c], high)
        field = wide[:64] + wide[64:] + dot(xi_tab[c, :64], low)
        for parity in range(2):
            for d in range(2):
                for k in range(2):
                    row = (d * 2 + k) * SLABS
                    gspec[pl.ds((2 * d + parity) * 384 + k * N + j, SLABS, stride=KZ), :] = field[
                        row : row + SLABS, 128 * parity : 128 * parity + 128
                    ]

    def turn_back(j, carry):
        value = total[block(j), :] + partial_x(j, 2)
        weight = kmat[pl.ds(pl.multiple_of(j * N, N), N), :]
        high, low = split(jnp.concatenate([value[:N] * weight, value[N:] * weight], axis=0))
        high_f[block(j), :] = high
        low_f[block(j), :] = low
        inverse_x(0, j, high, low)
        return carry

    def forward(c, carry):
        forward_y(c)

        @pl.when(c < 2)
        def _():
            def add(j, carry):
                total[block(j), :] = total[block(j), :] + partial_x(j, c)
                return carry

            lax.fori_loop(0, KZ, add, 0)

        return carry

    lax.fori_loop(0, CHUNKS, forward, 0)
    lax.fori_loop(0, KZ, turn_back, 0, unroll=2)

    def inverse_y(c, carry):
        @pl.when(c > 0)
        def _():
            def back_x(j, carry):
                inverse_x(c, j, high_f[block(j), :], low_f[block(j), :])
                return carry

            lax.fori_loop(0, KZ, back_x, 0)

        parts = []
        for k in range(2):
            wide = jnp.concatenate([gspec[pl.ds(l * 384 + k * N, N), :] for l in range(4)], axis=1)
            rows = slice(64, 320) if k == 0 else slice(0, 256)
            parts.append(triple(split(wide), (y_tab[0, rows], y_tab[1, rows]), ((1,), (1,))))
        tiles = [parts[0][:, :128], parts[0][:, 128:] + parts[1][:, :128], parts[1][:, 128:]]
        for l in range(3):
            send_b[pl.ds(c * 576 + l, N, stride=3), :] = tiles[l]
        send_all(send_b, recv_b, b_s, b_r, c)
        return carry

    lax.fori_loop(0, CHUNKS, inverse_y, 0)
    weight_copy.wait_recv()

    def ret_copy(c):
        rows = pl.ds(c * 288, 288)
        return pltpu.make_async_remote_copy(
            back.at[rows], landed.at[rows], ret_s.at[c], ret_r.at[c], device_id=(partner, me), device_id_type=MESH
        )

    def inverse_z(c, carry):
        wait_rows(recv_b, b_r.at[c], c * 576, 576)
        pad = jnp.zeros((64, 128), F32)
        turned = jnp.concatenate(
            [
                jnp.concatenate([recv_b[pl.ds(c * 576 + l, N, stride=3), :], pad], axis=0).T
                for l in range(3)
            ],
            axis=0,
        )
        back_z = z_back if crossing else z_tab
        both = triple(split(turned), (back_z[0], back_z[1]))

        def fields(start):
            first, second = [], []
            for r in range(4):
                ones, twos = [], []
                for k in range(2):
                    at = k * N + r * 24
                    re = both[at : at + 24, start : start + 256]
                    im = both[at + G : at + G + 24, start : start + 256]
                    ones.append(re[:, :G] - im[:, 128 : 128 + G])
                    twos.append(re[:, 128 : 128 + G] + im[:, :G])
                first.append(jnp.concatenate(ones, axis=0))
                second.append(jnp.concatenate(twos, axis=0))
            return jnp.concatenate(first, axis=1), jnp.concatenate(second, axis=1)

        first, second = fields(0)
        w_first = their_weights[pl.ds(upper, 1), :]
        w_second = their_weights[pl.ds(1 - upper, 1), :]
        mine = orbital(orb, c, 0), orbital(orb, c, 1)
        partners = orbital(theirs, c, upper), orbital(theirs, c, 1 - upper)
        if crossing:
            third, fourth = fields(256)
            swapped = upper == 1
            third, fourth = jnp.where(swapped, fourth, third), jnp.where(swapped, third, fourth)
        for l in range(3):
            lanes = slice(128 * l, 128 * l + 128)
            p0, p1 = w_first * partners[0][l], w_second * partners[1][l]
            m0, m1 = own_w0 * mine[0][l], own_w1 * mine[1][l]
            kept = [first[:, lanes] * p0, second[:, lanes] * p1]
            gone = [first[:, lanes] * m0, second[:, lanes] * m1]
            if crossing:
                kept[0] = kept[0] + fourth[:, lanes] * p1
                kept[1] = kept[1] + third[:, lanes] * p0
                gone[0] = gone[0] + third[:, lanes] * m1
                gone[1] = gone[1] + fourth[:, lanes] * m0
            for which, other in ((0, upper), (1, 1 - upper)):
                out[pl.ds(c * 288 + 2 * l + which, 48, stride=6), :] = -kept[which]
                back[pl.ds(c * 288 + 2 * l + other, 48, stride=6), :] = -gone[which]
        ret_copy(c).start()
        return carry

    lax.fori_loop(0, CHUNKS, inverse_z, 0)

    def finish(c, carry):
        ret_copy(c).wait_recv()
        rows = pl.ds(pl.multiple_of(c * 288, 288), 288)
        out[rows, :] = out[rows, :] + landed[rows, :]
        return carry

    lax.fori_loop(0, CHUNKS, finish, 0)

    weight_copy.wait_send()
    for c in range(CHUNKS):
        exch_copy(c).wait_send()
        ret_copy(c).wait_send()
        wait_rows(send_a, a_s.at[c], 0, 540)
        wait_rows(send_b, b_s.at[c], 0, 540)


def local(orbitals, occupation, kernel_hat, pair_mask):
    rows = orbitals.reshape(2, PLANES, 72, 128).transpose(1, 2, 0, 3).reshape(864, 128)
    consts = [jnp.asarray(value) for value in tables()]
    dma = pltpu.SemaphoreType.DMA

    def branch(mask):
        def run(rows, occupation, kernel_hat, *consts):
            return pl.pallas_call(
                functools.partial(kernel, mask),
                out_shape=jax.ShapeDtypeStruct((864, 128), F32),
                in_specs=[pl.BlockSpec(memory_space=pltpu.SMEM)] + [pl.BlockSpec(memory_space=pl.ANY)] * 6,
                out_specs=pl.BlockSpec(memory_space=pltpu.VMEM),
                scratch_shapes=[
                    pltpu.VMEM((864, 128), F32),
                    pltpu.VMEM((KZ, N * N), F32),
                    pltpu.VMEM((2, 256, 256), BF16),
                    pltpu.VMEM((2, 256, 512), BF16),
                    pltpu.VMEM((2, 320, 512), BF16),
                    pltpu.VMEM((CHUNKS, 384, N), BF16),
                    pltpu.VMEM((CHUNKS, 128, 384), BF16),
                    pltpu.VMEM((864, 128), F32),
                    pltpu.VMEM((8, 128), F32),
                    pltpu.VMEM((8, 128), F32),
                    pltpu.VMEM((384, 256), F32),
                    pltpu.VMEM((384, 256), F32),
                    pltpu.VMEM((1728, 128), F32),
                    pltpu.VMEM((1728, 128), F32),
                    pltpu.VMEM((1728, 128), F32),
                    pltpu.VMEM((1728, 128), F32),
                    pltpu.VMEM((1536, 128), F32),
                    pltpu.VMEM((1536, 128), F32),
                    pltpu.VMEM((KZ * 288, 128), F32),
                    pltpu.VMEM((KZ * N, 256), F32),
                    pltpu.VMEM((KZ * 384, 256), F32),
                    pltpu.VMEM((KZ * 384, 256), BF16),
                    pltpu.VMEM((KZ * 384, 256), BF16),
                    pltpu.VMEM((864, 128), F32),
                    pltpu.VMEM((864, 128), F32),
                    dma((6,)), dma((CHUNKS,)), dma((CHUNKS,)), dma, dma,
                    dma((CHUNKS,)), dma((CHUNKS,)), dma((CHUNKS,)), dma((CHUNKS,)),
                    dma((CHUNKS,)), dma((CHUNKS,)),
                ],
                compiler_params=pltpu.CompilerParams(
                    collective_id=mask, has_side_effects=True, vmem_limit_bytes=56 * 2**20
                ),
                name=f"exchange_{mask}",
            )(occupation, rows, kernel_hat, *consts)

        return run

    result = lax.switch(
        pair_mask[0] - 1, [branch(mask) for mask in range(1, 8)], rows, occupation, kernel_hat, *consts
    )
    planes = result.reshape(PLANES, 72, 2, 128).transpose(2, 0, 1, 3)
    planes = with_layout_constraint(planes, Layout((1, 2, 0, 3)))
    return planes.reshape(2, PLANES, G * G)


def solution(mesh):
    return jax.shard_map(
        local,
        mesh=mesh,
        in_specs=(P("grp", "slab", None), P("grp"), P("slab", None), P()),
        out_specs=P("grp", "slab", None),
        check_vma=False,
    )
```

```python
import functools
import math

import jax
import jax.numpy as jnp
import ml_dtypes
import numpy as np
from jax import lax
from jax.experimental import pallas as pl
from jax.experimental.layout import Layout, with_layout_constraint
from jax.experimental.pallas import tpu as pltpu
from jax.sharding import PartitionSpec as P

MESH = pl.DeviceIdType.MESH
G = 96
N = 192
PLANES = 6
CHUNKS = 3
SLABS = 16
KZ = 12
F32 = jnp.float32
BF16 = jnp.bfloat16


def halves(table):
    table = np.asarray(table, np.float64)
    high = table.astype(np.float32).astype(ml_dtypes.bfloat16)
    low = (table - high.astype(np.float64)).astype(np.float32).astype(ml_dtypes.bfloat16)
    return np.stack([high, low])


def rotation(freq, place):
    angle = 2.0 * math.pi * ((np.outer(freq, place)) % N) / N
    return np.cos(angle), np.sin(angle)


def tables():
    every = np.arange(N)
    z = np.arange(G)
    y = np.array([4 * q + r for r in range(4) for q in range(24)])
    cos_z, sin_z = rotation(every, z)
    z_both = np.zeros((N, 256))
    z_both[:, :G], z_both[:, 128 : 128 + G] = cos_z, sin_z
    y_fwd = np.zeros((2, G, 2, 2, 128))
    for parity in range(2):
        cos_y, sin_y = rotation(2 * np.arange(G) + parity, y)
        y_fwd[0, :, 0, parity, :G] = cos_y.T
        y_fwd[1, :, 0, parity, :G] = sin_y.T
        y_fwd[0, :, 1, parity, :G] = -sin_y.T
        y_fwd[1, :, 1, parity, :G] = cos_y.T
    x_fwd, x_inv = [], []
    for c in range(CHUNKS):
        cos_x, sin_x = rotation(every, np.array([PLANES * s + 2 * c + k for k in range(2) for s in range(SLABS)]))
        pair = halves(np.block([[cos_x, sin_x], [-sin_x, cos_x]]))
        x_fwd.append(np.concatenate([pair[0], pair[0], pair[1]], axis=1))
        x_inv.append(np.concatenate([pair[0].T, pair[1].T], axis=0))
    return [halves(z_both), halves(y_fwd.reshape(N, 512)), np.stack(x_fwd), np.stack(x_inv)]


STEPS = [(1, 2), (1, 0), (0, 1), (0, 3), (1, 1), (0, 2), (1, 3)]
PEERS = [(y, x, 0) for y, x in STEPS] + [(y, x, 1) for y, x in STEPS] + [(0, 0, 1)]


def split(value):
    high = value.astype(BF16)
    return high, (value - high.astype(F32)).astype(BF16)


def dot(left, right, contract=((1,), (0,))):
    return lax.dot_general(left, right, (contract, ((), ())), preferred_element_type=F32)


def triple(left, right, contract=((1,), (0,))):
    return (
        dot(left[0], right[0], contract)
        + dot(left[0], right[1], contract)
        + dot(left[1], right[0], contract)
    )


def kernel(
    mask,
    occ_ref, orb_in, kern_in, z_in, y_in, x_in, xi_in,
    out,
    orb, kern, z_tab, y_tab, x_tab, xi_tab,
    left_copy, right, pencils, send_a, recv_a, send_b, recv_b, spec, gspec, flat, kmat,
    total, high_f, low_f, left_terms, right_terms, left_in, right_in,
    in_s, exch_s, exch_r, a_s, a_r, b_s, b_r, ret_s, ret_r,
):
    grp = lax.axis_index("grp")
    me = lax.axis_index("slab")

    def flipped(bits):
        group = grp
        for bit in range(3):
            if bits >> bit & 1:
                group = group + (1 - 2 * (grp // 2**bit % 2)) * 2**bit
        return group

    mine_y, mine_x, mine_c = me // 8, me // 2 % 4, me % 2
    peers = [((mine_y + y) % 2 * 4 + (mine_x + x) % 4) * 2 + (mine_c + c) % 2 for y, x, c in PEERS]
    crossing = mask & 1
    partner, neighbour, diagonal = flipped(mask), flipped(1), flipped(mask ^ 1)
    field_group = grp + mine_y * (neighbour - grp) if crossing else grp
    upper = field_group // 2 ** (mask.bit_length() - 1) % 2
    groups = [neighbour if crossing and y else grp for y, _, c in PEERS]
    left = left_copy if crossing else orb
    if crossing:
        gather = [(0, orb, left, 0, None), (0, orb, right, 1, partner), (1, orb, left, 0, neighbour)]
        gather.append((1, orb, right, 1, None if mask == 1 else diagonal))
        scatter = [(0, right_terms, right_in, 1, partner), (1, left_terms, left_in, 0, neighbour)]
        if mask > 1:
            scatter.append((1, right_terms, right_in, 1, diagonal))
    else:
        gather = [(None, orb, right, 1, partner)]
        scatter = [(None, right_terms, right_in, 1, partner)]

    def on_half(half, run):
        if half is None:
            run()
        else:
            pl.when(mine_y == half)(run)

    def piece(c):
        return pl.ds(864, 8) if isinstance(c, int) and c == CHUNKS else pl.ds(c * 288, 288)

    def transfer(move, sems, c):
        _, source, target, side, group = move
        s_sem, r_sem = sems
        if group is None:
            return pltpu.make_async_copy(source.at[piece(c)], target.at[piece(c)], r_sem.at[side, c])
        return pltpu.make_async_remote_copy(
            source.at[piece(c)],
            target.at[piece(c)],
            s_sem.at[side, c],
            r_sem.at[side, c],
            device_id=(group, me),
            device_id_type=MESH,
        )

    def start(moves, sems, c):
        for half in (None, 0, 1):
            chosen = [move for move in moves if move[0] == half]

            def run(chosen=chosen):
                for move in chosen:
                    transfer(move, sems, c).start()

            if chosen:
                on_half(half, run)

    def drain(moves, sems, c):
        for half in (None, 0, 1):
            chosen = [move for move in moves if move[0] == half and move[4] is not None]

            def run(chosen=chosen):
                for move in chosen:
                    transfer(move, sems, c).wait_send()

            if chosen:
                on_half(half, run)

    def arrived(moves, sems, c):
        seen = {}
        for half, _, target, side, _ in moves:
            seen.setdefault(side, (target, []))[1].append(half)
        for side, (target, halves_) in seen.items():
            def run(side=side, target=target):
                rows = piece(c)
                pltpu.make_async_copy(target.at[rows], target.at[rows], sems[1].at[side, c]).wait()

            on_half(halves_[0] if len(halves_) == 1 else None, run)

    exch, ret = (exch_s, exch_r), (ret_s, ret_r)

    barrier = pltpu.get_barrier_semaphore()
    def greet(group):
        pl.semaphore_signal(barrier, inc=1, device_id=(group, me), device_id_type=MESH)

    met = SLABS
    if crossing:
        pl.when(mine_y == 0)(lambda: greet(partner))
        pl.when(mine_y == 1)(lambda: greet(neighbour))
        if mask > 1:
            pl.when(mine_y == 1)(lambda: greet(diagonal))
            met = SLABS + mine_y
    else:
        greet(partner)
    for group, peer in zip(groups, peers):
        pl.semaphore_signal(barrier, inc=1, device_id=(group, peer), device_id_type=MESH)

    stage = [
        pltpu.make_async_copy(source, target, in_s.at[i])
        for i, (source, target) in enumerate(
            (
                (orb_in, orb.at[pl.ds(0, 864)]),
                (kern_in, kern),
                (z_in, z_tab.at[:, pl.ds(0, N), :]),
                (y_in, y_tab.at[:, pl.ds(64, N), :]),
                (x_in, x_tab),
                (xi_in, xi_tab),
            )
        )
    ]
    for copy in stage:
        copy.start()
    which = lax.broadcasted_iota(jnp.int32, (8, 128), 0)
    orb[864:872, :] = jnp.where(which == 0, occ_ref[0].astype(F32), occ_ref[1].astype(F32)) * 0.25
    pencils[...] = jnp.zeros(pencils.shape, F32)
    total[...] = jnp.zeros(total.shape, F32)
    z_tab[:, N:, :] = jnp.zeros((2, 64, 256), BF16)
    y_tab[:, :64, :] = jnp.zeros((2, 64, 512), BF16)
    y_tab[:, 64 + N :, :] = jnp.zeros((2, 64, 512), BF16)
    stage[0].wait()
    pl.semaphore_wait(barrier, met)
    for c in range(CHUNKS + 1):
        start(gather, exch, c)

    stage[1].wait()

    def flatten(step, carry):
        for sub in range(8):
            m = step * 8 + sub
            flat[pl.ds(m, KZ, stride=288), :] = kern[:, pl.ds(pl.multiple_of(m * 128, 128), 128)] * (1.0 / N**3)
        return carry

    lax.fori_loop(0, 36, flatten, 0)

    def turn(j, carry):
        pad = jnp.zeros((32, 128), F32)
        t0, t1, t2 = [
            jnp.concatenate([flat[pl.ds(j * 288 + l, G, stride=3), :], pad], axis=0).T for l in range(3)
        ]
        base = pl.multiple_of(j * N, N)
        kmat[pl.ds(base, 128), 0:128] = t0
        kmat[pl.ds(base + 128, 64), 0:128] = t1[:64]
        kmat[pl.ds(base, 64), 128:256] = t1[64:]
        kmat[pl.ds(base + 64, 128), 128:256] = t2
        return carry

    lax.fori_loop(0, KZ, turn, 0)
    for copy in stage[2:]:
        copy.wait()
    def orbital(ref, c, which):
        return [ref[pl.ds(c * 288 + 2 * l + which, 48, stride=6), :] for l in range(3)]

    def send_all(sent, landing, s_sem, r_sem, c):
        for group, peer in zip(groups, peers):
            pltpu.make_async_remote_copy(
                sent.at[pl.ds(c * 576 + peer * 36, 36)],
                landing.at[pl.ds(c * 576 + me * 36, 36)],
                s_sem.at[c],
                r_sem.at[c],
                device_id=(group, peer),
                device_id_type=MESH,
            ).start()
        rows = pl.ds(c * 576 + me * 36, 36)
        pltpu.make_async_copy(sent.at[rows], landing.at[rows], r_sem.at[c]).start()

    def wait_rows(ref, sem, start, count):
        rows = pl.ds(start, count)
        pltpu.make_async_copy(ref.at[rows], ref.at[rows], sem).wait()

    def forward_z(c, carry):
        arrived(gather, exch, c)
        first = jnp.concatenate(
            [a * b for a, b in zip(orbital(left, c, 0), orbital(right, c, upper))], axis=1
        )
        second = jnp.concatenate(
            [a * b for a, b in zip(orbital(left, c, 1), orbital(right, c, 1 - upper))], axis=1
        )
        for r in range(4):
            for k in range(2):
                one = first[24 * k : 24 * k + 24, G * r : G * r + G]
                two = second[24 * k : 24 * k + 24, G * r : G * r + G]
                at = k * N + r * 24
                pencils[at : at + 24, 0:G] = one
                pencils[at : at + 24, 128 : 128 + G] = two
                pencils[at + G : at + G + 24, 0:G] = two
                pencils[at + G : at + G + 24, 128 : 128 + G] = -one
        spread = triple((z_tab[0, :N], z_tab[1, :N]), split(pencils[...]), ((1,), (1,)))
        for l in range(3):
            send_a[pl.ds(c * 576 + l, N, stride=3), :] = spread[:, 128 * l : 128 * l + 128]
        send_all(send_a, recv_a, a_s, a_r, c)
        return carry

    lax.fori_loop(0, CHUNKS, forward_z, 0)

    def forward_y(c):
        wait_rows(recv_a, a_r.at[c], c * 576, 576)
        wire = jnp.concatenate([recv_a[pl.ds(c * 576 + l, N, stride=3), :] for l in range(3)], axis=1)
        high, low = split(wire)
        for k in range(2):
            lanes = slice(128 * k, 128 * k + 256)
            rows = slice(64, 320) if k == 0 else slice(0, 256)
            result = triple((high[:, lanes], low[:, lanes]), (y_tab[0, rows], y_tab[1, rows]))
            for l in range(4):
                spec[pl.ds(l * 384 + k * N, N), :] = result[:, 128 * l : 128 * l + 128]

    def partial_x(j, c):
        field = jnp.concatenate(
            [
                jnp.concatenate(
                    [
                        spec[pl.ds((2 * d + parity) * 384 + k * N + j, SLABS, stride=KZ), :]
                        for d in range(2)
                        for k in range(2)
                    ],
                    axis=0,
                )
                for parity in range(2)
            ],
            axis=1,
        )
        high, low = split(field)
        return dot(x_tab[c], jnp.concatenate([high, low, high], axis=0))

    def block(j):
        return pl.ds(pl.multiple_of(j * 384, 384), 384)

    def inverse_x(c, j, high, low):
        wide = dot(xi_tab[c], high)
        field = wide[:64] + wide[64:] + dot(xi_tab[c, :64], low)
        for parity in range(2):
            for d in range(2):
                for k in range(2):
                    row = (d * 2 + k) * SLABS
                    gspec[pl.ds((2 * d + parity) * 384 + k * N + j, SLABS, stride=KZ), :] = field[
                        row : row + SLABS, 128 * parity : 128 * parity + 128
                    ]

    def turn_back(j, carry):
        value = total[block(j), :] + partial_x(j, 2)
        weight = kmat[pl.ds(pl.multiple_of(j * N, N), N), :]
        high, low = split(jnp.concatenate([value[:N] * weight, value[N:] * weight], axis=0))
        high_f[block(j), :] = high
        low_f[block(j), :] = low
        inverse_x(0, j, high, low)
        return carry

    def forward(c, carry):
        forward_y(c)

        @pl.when(c < 2)
        def _():
            def add(j, carry):
                total[block(j), :] = total[block(j), :] + partial_x(j, c)
                return carry

            lax.fori_loop(0, KZ, add, 0)

        return carry

    lax.fori_loop(0, CHUNKS, forward, 0)
    lax.fori_loop(0, KZ, turn_back, 0, unroll=2)

    def inverse_y(c, carry):
        @pl.when(c > 0)
        def _():
            def back_x(j, carry):
                inverse_x(c, j, high_f[block(j), :], low_f[block(j), :])
                return carry

            lax.fori_loop(0, KZ, back_x, 0)

        parts = []
        for k in range(2):
            wide = jnp.concatenate([gspec[pl.ds(l * 384 + k * N, N), :] for l in range(4)], axis=1)
            rows = slice(64, 320) if k == 0 else slice(0, 256)
            parts.append(triple(split(wide), (y_tab[0, rows], y_tab[1, rows]), ((1,), (1,))))
        tiles = [parts[0][:, :128], parts[0][:, 128:] + parts[1][:, :128], parts[1][:, 128:]]
        for l in range(3):
            send_b[pl.ds(c * 576 + l, N, stride=3), :] = tiles[l]
        send_all(send_b, recv_b, b_s, b_r, c)
        return carry

    lax.fori_loop(0, CHUNKS, inverse_y, 0)
    arrived(gather, exch, CHUNKS)

    def inverse_z(c, carry):
        wait_rows(recv_b, b_r.at[c], c * 576, 576)
        pad = jnp.zeros((64, 128), F32)
        turned = jnp.concatenate(
            [
                jnp.concatenate([recv_b[pl.ds(c * 576 + l, N, stride=3), :], pad], axis=0).T
                for l in range(3)
            ],
            axis=0,
        )
        both = triple(split(turned), (z_tab[0], z_tab[1]))
        first, second = [], []
        for r in range(4):
            ones, twos = [], []
            for k in range(2):
                at = k * N + r * 24
                re = both[at : at + 24]
                im = both[at + G : at + G + 24]
                ones.append(re[:, :G] - im[:, 128 : 128 + G])
                twos.append(re[:, 128 : 128 + G] + im[:, :G])
            first.append(jnp.concatenate(ones, axis=0))
            second.append(jnp.concatenate(twos, axis=0))
        first = jnp.concatenate(first, axis=1)
        second = jnp.concatenate(second, axis=1)
        for field, which, other in ((first, 0, upper), (second, 1, 1 - upper)):
            near, far = orbital(left, c, which), orbital(right, c, other)
            near_w, far_w = left[pl.ds(864 + which, 1), :], right[pl.ds(864 + other, 1), :]
            for l in range(3):
                tile = field[:, 128 * l : 128 * l + 128]
                left_terms[pl.ds(c * 288 + 2 * l + which, 48, stride=6), :] = -(far_w * tile * far[l])
                right_terms[pl.ds(c * 288 + 2 * l + other, 48, stride=6), :] = -(near_w * tile * near[l])
        start(scatter, ret, c)
        return carry

    lax.fori_loop(0, CHUNKS, inverse_z, 0)

    def finish(c, carry):
        arrived(scatter, ret, c)
        rows = pl.ds(pl.multiple_of(c * 288, 288), 288)

        def lower():
            out[rows, :] = left_terms[rows, :] + right_in[rows, :]

        def higher():
            out[rows, :] = left_in[rows, :] + (right_terms if mask == 1 else right_in)[rows, :]

        if crossing:
            pl.when(mine_y == 0)(lower)
            pl.when(mine_y == 1)(higher)
        else:
            lower()
        return carry

    lax.fori_loop(0, CHUNKS, finish, 0)

    drain(gather, exch, CHUNKS)
    for c in range(CHUNKS):
        drain(gather, exch, c)
        drain(scatter, ret, c)
        wait_rows(send_a, a_s.at[c], 0, 540)
        wait_rows(send_b, b_s.at[c], 0, 540)


def local(orbitals, occupation, kernel_hat, pair_mask):
    rows = orbitals.reshape(2, PLANES, 72, 128).transpose(1, 2, 0, 3).reshape(864, 128)
    consts = [jnp.asarray(value) for value in tables()]
    dma = pltpu.SemaphoreType.DMA

    def branch(mask):
        def run(rows, occupation, kernel_hat, *consts):
            return pl.pallas_call(
                functools.partial(kernel, mask),
                out_shape=jax.ShapeDtypeStruct((864, 128), F32),
                in_specs=[pl.BlockSpec(memory_space=pltpu.SMEM)] + [pl.BlockSpec(memory_space=pl.ANY)] * 6,
                out_specs=pl.BlockSpec(memory_space=pltpu.VMEM),
                scratch_shapes=[
                    pltpu.VMEM((872, 128), F32),
                    pltpu.VMEM((KZ, N * N), F32),
                    pltpu.VMEM((2, 256, 256), BF16),
                    pltpu.VMEM((2, 320, 512), BF16),
                    pltpu.VMEM((CHUNKS, 384, N), BF16),
                    pltpu.VMEM((CHUNKS, 128, 384), BF16),
                    pltpu.VMEM((872, 128), F32),
                    pltpu.VMEM((872, 128), F32),
                    pltpu.VMEM((384, 256), F32),
                    pltpu.VMEM((1728, 128), F32),
                    pltpu.VMEM((1728, 128), F32),
                    pltpu.VMEM((1728, 128), F32),
                    pltpu.VMEM((1728, 128), F32),
                    pltpu.VMEM((1536, 128), F32),
                    pltpu.VMEM((1536, 128), F32),
                    pltpu.VMEM((KZ * 288, 128), F32),
                    pltpu.VMEM((KZ * N, 256), F32),
                    pltpu.VMEM((KZ * 384, 256), F32),
                    pltpu.VMEM((KZ * 384, 256), BF16),
                    pltpu.VMEM((KZ * 384, 256), BF16),
                    pltpu.VMEM((864, 128), F32),
                    pltpu.VMEM((864, 128), F32),
                    pltpu.VMEM((864, 128), F32),
                    pltpu.VMEM((864, 128), F32),
                    dma((6,)), dma((2, CHUNKS + 1)), dma((2, CHUNKS + 1)),
                    dma((CHUNKS,)), dma((CHUNKS,)), dma((CHUNKS,)), dma((CHUNKS,)),
                    dma((2, CHUNKS)), dma((2, CHUNKS)),
                ],
                compiler_params=pltpu.CompilerParams(
                    collective_id=mask, has_side_effects=True, vmem_limit_bytes=56 * 2**20
                ),
                name=f"exchange_{mask}",
            )(occupation, rows, kernel_hat, *consts)

        return run

    result = lax.switch(
        pair_mask[0] - 1, [branch(mask) for mask in range(1, 8)], rows, occupation, kernel_hat, *consts
    )
    planes = result.reshape(PLANES, 72, 2, 128).transpose(2, 0, 1, 3)
    planes = with_layout_constraint(planes, Layout((1, 2, 0, 3)))
    return planes.reshape(2, PLANES, G * G)


def solution(mesh):
    return jax.shard_map(
        local,
        mesh=mesh,
        in_specs=(P("grp", "slab", None), P("grp"), P("slab", None), P()),
        out_specs=P("grp", "slab", None),
        check_vma=False,
    )
```

```python
import functools
import math

import jax
import jax.numpy as jnp
import ml_dtypes
import numpy as np
from jax import lax
from jax.experimental import pallas as pl
from jax.experimental.layout import Layout, with_layout_constraint
from jax.experimental.pallas import tpu as pltpu
from jax.sharding import PartitionSpec as P

MESH = pl.DeviceIdType.MESH
G = 96
N = 192
PLANES = 6
CHUNKS = 3
SLABS = 16
KZ = 12
F32 = jnp.float32
BF16 = jnp.bfloat16


def halves(table):
    table = np.asarray(table, np.float64)
    high = table.astype(np.float32).astype(ml_dtypes.bfloat16)
    low = (table - high.astype(np.float64)).astype(np.float32).astype(ml_dtypes.bfloat16)
    return np.stack([high, low])


def rotation(freq, place):
    angle = 2.0 * math.pi * ((np.outer(freq, place)) % N) / N
    return np.cos(angle), np.sin(angle)


def tables():
    every = np.arange(N)
    z = np.arange(G)
    y = np.array([4 * q + r for r in range(4) for q in range(24)])
    cos_z, sin_z = rotation(every, z)
    z_both = np.zeros((N, 256))
    z_both[:, :G], z_both[:, 128 : 128 + G] = cos_z, sin_z
    y_fwd = np.zeros((2, G, 2, 2, 128))
    for parity in range(2):
        cos_y, sin_y = rotation(2 * np.arange(G) + parity, y)
        y_fwd[0, :, 0, parity, :G] = cos_y.T
        y_fwd[1, :, 0, parity, :G] = sin_y.T
        y_fwd[0, :, 1, parity, :G] = -sin_y.T
        y_fwd[1, :, 1, parity, :G] = cos_y.T
    x_fwd, x_inv = [], []
    for c in range(CHUNKS):
        cos_x, sin_x = rotation(every, np.array([PLANES * s + 2 * c + k for k in range(2) for s in range(SLABS)]))
        pair = halves(np.block([[cos_x, sin_x], [-sin_x, cos_x]]))
        x_fwd.append(np.concatenate([pair[0], pair[0], pair[1]], axis=1))
        x_inv.append(np.concatenate([pair[0].T, pair[1].T], axis=0))
    return [halves(z_both), halves(y_fwd.reshape(N, 512)), np.stack(x_fwd), np.stack(x_inv)]


STEPS = [(1, 2), (1, 0), (0, 1), (0, 3), (1, 1), (0, 2), (1, 3)]
PEERS = [(y, x, 0) for y, x in STEPS] + [(y, x, 1) for y, x in STEPS] + [(0, 0, 1)]


def split(value):
    high = value.astype(BF16)
    return high, (value - high.astype(F32)).astype(BF16)


def dot(left, right, contract=((1,), (0,))):
    return lax.dot_general(left, right, (contract, ((), ())), preferred_element_type=F32)


def triple(left, right, contract=((1,), (0,))):
    return (
        dot(left[0], right[0], contract)
        + dot(left[0], right[1], contract)
        + dot(left[1], right[0], contract)
    )


def kernel(
    mask,
    occ_ref, orb_in, kern_in, z_in, y_in, x_in, xi_in,
    out,
    orb, kern, z_tab, y_tab, x_tab, xi_tab,
    left_copy, right, pencils, send_a, recv_a, send_b, recv_b, spec, gspec, flat, kmat,
    total, high_f, low_f, left_terms, right_terms, left_in, right_in,
    in_s, exch_s, exch_r, a_s, a_r, b_s, b_r, ret_s, ret_r,
):
    grp = lax.axis_index("grp")
    me = lax.axis_index("slab")

    def flipped(bits):
        group = grp
        for bit in range(3):
            if bits >> bit & 1:
                group = group + (1 - 2 * (grp // 2**bit % 2)) * 2**bit
        return group

    mine_y, mine_x, mine_c = me // 8, me // 2 % 4, me % 2
    peers = [((mine_y + y) % 2 * 4 + (mine_x + x) % 4) * 2 + (mine_c + c) % 2 for y, x, c in PEERS]
    crossing = mask & 1
    partner, neighbour, diagonal = flipped(mask), flipped(1), flipped(mask ^ 1)
    field_group = grp + mine_y * (neighbour - grp) if crossing else grp
    upper = field_group // 2 ** (mask.bit_length() - 1) % 2
    groups = [neighbour if crossing and y else grp for y, _, c in PEERS]
    left = left_copy if crossing else orb
    if crossing:
        gather = [(0, orb, left, 0, None), (0, orb, right, 1, partner), (1, orb, left, 0, neighbour)]
        gather.append((1, orb, right, 1, None if mask == 1 else diagonal))
        scatter = [(0, right_terms, right_in, 1, partner), (1, left_terms, left_in, 0, neighbour)]
        if mask > 1:
            scatter.append((1, right_terms, right_in, 1, diagonal))
    else:
        gather = [(None, orb, right, 1, partner)]
        scatter = [(None, right_terms, right_in, 1, partner)]

    def on_half(half, run):
        if half is None:
            run()
        else:
            pl.when(mine_y == half)(run)

    def piece(c):
        return pl.ds(864, 8) if isinstance(c, int) and c == CHUNKS else pl.ds(c * 288, 288)

    def transfer(move, sems, c):
        _, source, target, side, group = move
        s_sem, r_sem = sems
        if group is None:
            return pltpu.make_async_copy(source.at[piece(c)], target.at[piece(c)], r_sem.at[side, c])
        return pltpu.make_async_remote_copy(
            source.at[piece(c)],
            target.at[piece(c)],
            s_sem.at[side, c],
            r_sem.at[side, c],
            device_id=(group, me),
            device_id_type=MESH,
        )

    def start(moves, sems, c):
        for half in (None, 0, 1):
            chosen = [move for move in moves if move[0] == half]

            def run(chosen=chosen):
                for move in chosen:
                    transfer(move, sems, c).start()

            if chosen:
                on_half(half, run)

    def drain(moves, sems, c):
        for half in (None, 0, 1):
            chosen = [move for move in moves if move[0] == half and move[4] is not None]

            def run(chosen=chosen):
                for move in chosen:
                    transfer(move, sems, c).wait_send()

            if chosen:
                on_half(half, run)

    def arrived(moves, sems, c):
        seen = {}
        for half, _, target, side, _ in moves:
            seen.setdefault(side, (target, []))[1].append(half)
        for side, (target, halves_) in seen.items():
            def run(side=side, target=target):
                rows = piece(c)
                pltpu.make_async_copy(target.at[rows], target.at[rows], sems[1].at[side, c]).wait()

            on_half(halves_[0] if len(halves_) == 1 else None, run)

    exch, ret = (exch_s, exch_r), (ret_s, ret_r)

    barrier = pltpu.get_barrier_semaphore()
    def greet(group):
        pl.semaphore_signal(barrier, inc=1, device_id=(group, me), device_id_type=MESH)

    met = SLABS
    if crossing:
        pl.when(mine_y == 0)(lambda: greet(partner))
        pl.when(mine_y == 1)(lambda: greet(neighbour))
        if mask > 1:
            pl.when(mine_y == 1)(lambda: greet(diagonal))
            met = SLABS + mine_y
    else:
        greet(partner)
    for group, peer in zip(groups, peers):
        pl.semaphore_signal(barrier, inc=1, device_id=(group, peer), device_id_type=MESH)

    stage = [
        pltpu.make_async_copy(source, target, in_s.at[i])
        for i, (source, target) in enumerate(
            (
                (orb_in, orb.at[pl.ds(0, 864)]),
                (kern_in, kern),
                (z_in, z_tab.at[:, pl.ds(0, N), :]),
                (y_in, y_tab.at[:, pl.ds(64, N), :]),
                (x_in, x_tab),
                (xi_in, xi_tab),
            )
        )
    ]
    for copy in stage:
        copy.start()
    which = lax.broadcasted_iota(jnp.int32, (8, 128), 0)
    orb[864:872, :] = jnp.where(which == 0, occ_ref[0].astype(F32), occ_ref[1].astype(F32)) * 0.25
    pencils[...] = jnp.zeros(pencils.shape, F32)

    def clear(step, carry):
        total[pl.ds(pl.multiple_of(step * 96, 96), 96), :] = jnp.zeros((96, 256), F32)
        return carry

    lax.fori_loop(0, 48, clear, 0)
    z_tab[:, N:, :] = jnp.zeros((2, 64, 256), BF16)
    y_tab[:, :64, :] = jnp.zeros((2, 64, 512), BF16)
    y_tab[:, 64 + N :, :] = jnp.zeros((2, 64, 512), BF16)
    stage[0].wait()
    pl.semaphore_wait(barrier, met)
    for c in range(CHUNKS + 1):
        start(gather, exch, c)

    stage[1].wait()

    def flatten(step, carry):
        for sub in range(8):
            m = step * 8 + sub
            flat[pl.ds(m, KZ, stride=288), :] = kern[:, pl.ds(pl.multiple_of(m * 128, 128), 128)] * (1.0 / N**3)
        return carry

    lax.fori_loop(0, 36, flatten, 0)

    def turn(j, carry):
        pad = jnp.zeros((32, 128), F32)
        t0, t1, t2 = [
            jnp.concatenate([flat[pl.ds(j * 288 + l, G, stride=3), :], pad], axis=0).T for l in range(3)
        ]
        base = pl.multiple_of(j * N, N)
        kmat[pl.ds(base, 128), 0:128] = t0
        kmat[pl.ds(base + 128, 64), 0:128] = t1[:64]
        kmat[pl.ds(base, 64), 128:256] = t1[64:]
        kmat[pl.ds(base + 64, 128), 128:256] = t2
        return carry

    lax.fori_loop(0, KZ, turn, 0)
    for copy in stage[2:]:
        copy.wait()
    def orbital(ref, c, which):
        return [ref[pl.ds(c * 288 + 2 * l + which, 48, stride=6), :] for l in range(3)]

    def send_all(sent, landing, s_sem, r_sem, c):
        for group, peer in zip(groups, peers):
            pltpu.make_async_remote_copy(
                sent.at[pl.ds(c * 576 + peer * 36, 36)],
                landing.at[pl.ds(c * 576 + me * 36, 36)],
                s_sem.at[c],
                r_sem.at[c],
                device_id=(group, peer),
                device_id_type=MESH,
            ).start()
        rows = pl.ds(c * 576 + me * 36, 36)
        pltpu.make_async_copy(sent.at[rows], landing.at[rows], r_sem.at[c]).start()

    def wait_rows(ref, sem, start, count):
        rows = pl.ds(start, count)
        pltpu.make_async_copy(ref.at[rows], ref.at[rows], sem).wait()

    def forward_z(c, carry):
        arrived(gather, exch, c)
        first = jnp.concatenate(
            [a * b for a, b in zip(orbital(left, c, 0), orbital(right, c, upper))], axis=1
        )
        second = jnp.concatenate(
            [a * b for a, b in zip(orbital(left, c, 1), orbital(right, c, 1 - upper))], axis=1
        )
        for r in range(4):
            for k in range(2):
                one = first[24 * k : 24 * k + 24, G * r : G * r + G]
                two = second[24 * k : 24 * k + 24, G * r : G * r + G]
                at = k * N + r * 24
                pencils[at : at + 24, 0:G] = one
                pencils[at : at + 24, 128 : 128 + G] = two
                pencils[at + G : at + G + 24, 0:G] = two
                pencils[at + G : at + G + 24, 128 : 128 + G] = -one
        spread = triple((z_tab[0, :N], z_tab[1, :N]), split(pencils[...]), ((1,), (1,)))
        for l in range(3):
            send_a[pl.ds(c * 576 + l, N, stride=3), :] = spread[:, 128 * l : 128 * l + 128]
        send_all(send_a, recv_a, a_s, a_r, c)
        return carry

    lax.fori_loop(0, CHUNKS, forward_z, 0)

    def forward_y(c):
        wait_rows(recv_a, a_r.at[c], c * 576, 576)
        wire = jnp.concatenate([recv_a[pl.ds(c * 576 + l, N, stride=3), :] for l in range(3)], axis=1)
        high, low = split(wire)
        for k in range(2):
            lanes = slice(128 * k, 128 * k + 256)
            rows = slice(64, 320) if k == 0 else slice(0, 256)
            result = triple((high[:, lanes], low[:, lanes]), (y_tab[0, rows], y_tab[1, rows]))
            for l in range(4):
                spec[pl.ds(l * 384 + k * N, N), :] = result[:, 128 * l : 128 * l + 128]

    def partial_x(j, c):
        field = jnp.concatenate(
            [
                jnp.concatenate(
                    [
                        spec[pl.ds((2 * d + parity) * 384 + k * N + j, SLABS, stride=KZ), :]
                        for d in range(2)
                        for k in range(2)
                    ],
                    axis=0,
                )
                for parity in range(2)
            ],
            axis=1,
        )
        high, low = split(field)
        return dot(x_tab[c], jnp.concatenate([high, low, high], axis=0))

    def block(j):
        return pl.ds(pl.multiple_of(j * 384, 384), 384)

    def inverse_x(c, j, high, low):
        wide = dot(xi_tab[c], high)
        field = wide[:64] + wide[64:] + dot(xi_tab[c, :64], low)
        for parity in range(2):
            for d in range(2):
                for k in range(2):
                    row = (d * 2 + k) * SLABS
                    gspec[pl.ds((2 * d + parity) * 384 + k * N + j, SLABS, stride=KZ), :] = field[
                        row : row + SLABS, 128 * parity : 128 * parity + 128
                    ]

    def turn_back(j, carry):
        value = total[block(j), :] + partial_x(j, 2)
        weight = kmat[pl.ds(pl.multiple_of(j * N, N), N), :]
        high, low = split(jnp.concatenate([value[:N] * weight, value[N:] * weight], axis=0))
        high_f[block(j), :] = high
        low_f[block(j), :] = low
        inverse_x(0, j, high, low)
        return carry

    def forward(c, carry):
        forward_y(c)

        @pl.when(c < 2)
        def _():
            def add(j, carry):
                total[block(j), :] = total[block(j), :] + partial_x(j, c)
                return carry

            lax.fori_loop(0, KZ, add, 0)

        return carry

    lax.fori_loop(0, CHUNKS, forward, 0)
    lax.fori_loop(0, KZ, turn_back, 0, unroll=6)

    def inverse_y(c, carry):
        @pl.when(c > 0)
        def _():
            def back_x(j, carry):
                inverse_x(c, j, high_f[block(j), :], low_f[block(j), :])
                return carry

            lax.fori_loop(0, KZ, back_x, 0)

        parts = []
        for k in range(2):
            wide = jnp.concatenate([gspec[pl.ds(l * 384 + k * N, N), :] for l in range(4)], axis=1)
            rows = slice(64, 320) if k == 0 else slice(0, 256)
            parts.append(triple(split(wide), (y_tab[0, rows], y_tab[1, rows]), ((1,), (1,))))
        tiles = [parts[0][:, :128], parts[0][:, 128:] + parts[1][:, :128], parts[1][:, 128:]]
        for l in range(3):
            send_b[pl.ds(c * 576 + l, N, stride=3), :] = tiles[l]
        send_all(send_b, recv_b, b_s, b_r, c)
        return carry

    lax.fori_loop(0, CHUNKS, inverse_y, 0)
    arrived(gather, exch, CHUNKS)

    def inverse_z(c, carry):
        wait_rows(recv_b, b_r.at[c], c * 576, 576)
        pad = jnp.zeros((64, 128), F32)
        turned = jnp.concatenate(
            [
                jnp.concatenate([recv_b[pl.ds(c * 576 + l, N, stride=3), :], pad], axis=0).T
                for l in range(3)
            ],
            axis=0,
        )
        both = triple(split(turned), (z_tab[0], z_tab[1]))
        first, second = [], []
        for r in range(4):
            ones, twos = [], []
            for k in range(2):
                at = k * N + r * 24
                re = both[at : at + 24]
                im = both[at + G : at + G + 24]
                ones.append(re[:, :G] - im[:, 128 : 128 + G])
                twos.append(re[:, 128 : 128 + G] + im[:, :G])
            first.append(jnp.concatenate(ones, axis=0))
            second.append(jnp.concatenate(twos, axis=0))
        first = jnp.concatenate(first, axis=1)
        second = jnp.concatenate(second, axis=1)
        for field, which, other in ((first, 0, upper), (second, 1, 1 - upper)):
            near, far = orbital(left, c, which), orbital(right, c, other)
            near_w, far_w = left[pl.ds(864 + which, 1), :], right[pl.ds(864 + other, 1), :]
            for l in range(3):
                tile = field[:, 128 * l : 128 * l + 128]
                left_terms[pl.ds(c * 288 + 2 * l + which, 48, stride=6), :] = -(far_w * tile * far[l])
                right_terms[pl.ds(c * 288 + 2 * l + other, 48, stride=6), :] = -(near_w * tile * near[l])
        start(scatter, ret, c)
        return carry

    lax.fori_loop(0, CHUNKS, inverse_z, 0)

    def finish(c, carry):
        arrived(scatter, ret, c)
        rows = pl.ds(pl.multiple_of(c * 288, 288), 288)

        def lower():
            out[rows, :] = left_terms[rows, :] + right_in[rows, :]

        def higher():
            out[rows, :] = left_in[rows, :] + (right_terms if mask == 1 else right_in)[rows, :]

        if crossing:
            pl.when(mine_y == 0)(lower)
            pl.when(mine_y == 1)(higher)
        else:
            lower()
        return carry

    lax.fori_loop(0, CHUNKS, finish, 0)

    drain(gather, exch, CHUNKS)
    for c in range(CHUNKS):
        drain(gather, exch, c)
        drain(scatter, ret, c)
        wait_rows(send_a, a_s.at[c], 0, 540)
        wait_rows(send_b, b_s.at[c], 0, 540)


def local(orbitals, occupation, kernel_hat, pair_mask):
    rows = orbitals.reshape(2, PLANES, 72, 128).transpose(1, 2, 0, 3).reshape(864, 128)
    consts = [jnp.asarray(value) for value in tables()]
    dma = pltpu.SemaphoreType.DMA

    def branch(mask):
        def run(rows, occupation, kernel_hat, *consts):
            return pl.pallas_call(
                functools.partial(kernel, mask),
                out_shape=jax.ShapeDtypeStruct((864, 128), F32),
                in_specs=[pl.BlockSpec(memory_space=pltpu.SMEM)] + [pl.BlockSpec(memory_space=pl.ANY)] * 6,
                out_specs=pl.BlockSpec(memory_space=pltpu.VMEM),
                scratch_shapes=[
                    pltpu.VMEM((872, 128), F32),
                    pltpu.VMEM((KZ, N * N), F32),
                    pltpu.VMEM((2, 256, 256), BF16),
                    pltpu.VMEM((2, 320, 512), BF16),
                    pltpu.VMEM((CHUNKS, 384, N), BF16),
                    pltpu.VMEM((CHUNKS, 128, 384), BF16),
                    pltpu.VMEM((872, 128), F32),
                    pltpu.VMEM((872, 128), F32),
                    pltpu.VMEM((384, 256), F32),
                    pltpu.VMEM((1728, 128), F32),
                    pltpu.VMEM((1728, 128), F32),
                    pltpu.VMEM((1728, 128), F32),
                    pltpu.VMEM((1728, 128), F32),
                    pltpu.VMEM((1536, 128), F32),
                    pltpu.VMEM((1536, 128), F32),
                    pltpu.VMEM((KZ * 288, 128), F32),
                    pltpu.VMEM((KZ * N, 256), F32),
                    pltpu.VMEM((KZ * 384, 256), F32),
                    pltpu.VMEM((KZ * 384, 256), BF16),
                    pltpu.VMEM((KZ * 384, 256), BF16),
                    pltpu.VMEM((864, 128), F32),
                    pltpu.VMEM((864, 128), F32),
                    pltpu.VMEM((864, 128), F32),
                    pltpu.VMEM((864, 128), F32),
                    dma((6,)), dma((2, CHUNKS + 1)), dma((2, CHUNKS + 1)),
                    dma((CHUNKS,)), dma((CHUNKS,)), dma((CHUNKS,)), dma((CHUNKS,)),
                    dma((2, CHUNKS)), dma((2, CHUNKS)),
                ],
                compiler_params=pltpu.CompilerParams(
                    collective_id=mask, has_side_effects=True, vmem_limit_bytes=56 * 2**20
                ),
                name=f"exchange_{mask}",
            )(occupation, rows, kernel_hat, *consts)

        return run

    result = lax.switch(
        pair_mask[0] - 1, [branch(mask) for mask in range(1, 8)], rows, occupation, kernel_hat, *consts
    )
    planes = result.reshape(PLANES, 72, 2, 128).transpose(2, 0, 1, 3)
    planes = with_layout_constraint(planes, Layout((1, 2, 0, 3)))
    return planes.reshape(2, PLANES, G * G)


def solution(mesh):
    return jax.shard_map(
        local,
        mesh=mesh,
        in_specs=(P("grp", "slab", None), P("grp"), P("slab", None), P()),
        out_specs=P("grp", "slab", None),
        check_vma=False,
    )
```
